32 devices in a mesh: space: 32 (over z, y, x, core), mem: 1.
Axes of the slice: x: 2, y: 2, z: 4, core: 2. Of those that a mesh axis runs over, the one named last changes fastest.
Arguments:
- members: bfloat16 [128, 768, 2, 384], P(('space', 'mem')), may hold values from -6 to 6
- state: float32 [768, 2, 384], P('space'), may hold values from -6 to 6
- cotangent: float32 [768, 2, 384], P('space'), may hold values from -6 to 6
- conv_in: float32 [3, 3, 128, 2], replicated, may hold values from -1.5 to 1.5
- conv_out: float32 [3, 3, 2, 128], replicated, may hold values from -0.1875 to 0.1875
- bias: float32 [128], replicated, may hold values from -3 to 3
Outputs:
- increment: float32 [768, 2, 384], P('space')
- response: float32 [768, 2, 384], P('space')
The draws below stay inside these ranges and needn't reach their ends.
All inputs are finite; a program needn't handle non-finite values.
Results may differ from the reference program's by a relative error of at most 0.0045.
Values may be sent and summed in bfloat16 or wider, within the bound.
A program may use at most 64 MiB of HBM per device.

```python
import jax
import jax.numpy as jnp
from jax import lax

LAT = 384
HID = 128
VARS = 2
HALF = 16
LON = 768
MEMBERS = 128


def strengthened(drawn, own_key, source, target, shards_of, factor):
    owner, partner = [(jnp.arange(drawn.shape[axis_at]) // (drawn.shape[axis_at] // shards_of)).reshape([-1 if axis == axis_at else 1 for axis in range(drawn.ndim)]) for axis_at in (source, target)]
    chosen = jax.random.permutation(own_key, shards_of)[partner]
    strong = (owner == chosen) | (owner == (partner + shards_of // 2) % shards_of)
    return jnp.where(strong, factor * drawn, drawn)


def block_scale(rng, shape, shards, low, largest):
    level = 1.0
    for dim, parts in shards:
        steps = jax.random.uniform(jax.random.fold_in(jax.random.fold_in(rng, 6), dim), (parts,), jnp.float32, low / len(shards), largest / len(shards))
        level = level * jnp.repeat(jnp.exp(steps), shape[dim] // parts).reshape((-1,) + (1,) * (len(shape) - 1 - dim))
    return level


def centred(rng, shape, scale, limit, shards=(), kind=jnp.bfloat16):
    result = scale * jax.random.normal(rng, shape, jnp.float32)
    if shards:
        result = result * block_scale(rng, shape, shards, -0.22, 0.18)
    return jnp.clip(result, -limit, limit).astype(kind)


def gaussian_with(stream_key, shape, scale, reach, pieces, heavy, dtype=jnp.bfloat16):
    drawn = scale * jax.random.normal(stream_key, shape, jnp.float32)
    if pieces:
        drawn = drawn * block_scale(stream_key, shape, pieces, -0.22, 0.18)
    return jnp.clip(strengthened(drawn, jax.random.fold_in(stream_key, 3), *heavy), -reach, reach).astype(dtype)


def setup_inputs(seed: int = 0) -> dict:
    splits = jax.random.split(jax.random.key(seed), 7)
    return {
        "members": gaussian_with(splits[0], (MEMBERS, LON, VARS, LAT), 1.0, 6.0, ((0, 32),), (0, 1, 32, 2.75)),
        "state": centred(splits[1], (LON, VARS, LAT), 1.0, 6.0, ((0, 32),), jnp.float32),
        "cotangent": centred(splits[2], (LON, VARS, LAT), 1.0, 6.0, ((0, 32),), jnp.float32),
        "conv_in": centred(splits[3], (3, 3, HID, VARS), (9 * VARS) ** -0.5, 1.5, (), jnp.float32),
        "conv_out": centred(splits[4], (3, 3, VARS, HID), (9 * HID) ** -0.5, 0.1875, (), jnp.float32),
        "bias": centred(splits[5], (HID,), 0.5, 3.0, (), jnp.float32),
    }


def wrap_lon(field):
    return jnp.concatenate([field[-1:], field, field[:1]], axis=0)


def convolve(field, weight):
    padded = jnp.pad(wrap_lon(field), ((0, 0), (0, 0), (1, 1)))
    row_count = field.shape[0]
    lat_count = field.shape[2]
    summed = jnp.zeros((row_count, weight.shape[2], lat_count), jnp.float32)
    for step_lon in range(3):
        for step_lat in range(3):
            window = padded[step_lon:step_lon + row_count, :, step_lat:step_lat + lat_count]
            summed = summed + jnp.einsum("oc,xcy->xoy", weight[step_lon, step_lat], window, precision=lax.Precision.HIGHEST)
    return summed


def flipped(weight):
    return jnp.transpose(weight[::-1, ::-1], (0, 1, 3, 2))


def band_matrix(count, wrap):
    row_index = jnp.arange(count)[:, None]
    col_index = jnp.arange(count)[None, :]
    distance = jnp.abs(row_index - col_index)
    if wrap:
        distance = jnp.minimum(distance, count - distance)
    ratio = distance.astype(jnp.float32) / (HALF + 1.0)
    return jnp.where(distance <= HALF, 1.0 - ratio * ratio, 0.0).astype(jnp.bfloat16)


def reference(members, state, cotangent, conv_in, conv_out, bias):
    activity = jnp.tanh(convolve(state, conv_in) + bias[None, :, None])
    slopes = 1.0 - activity * activity
    backward = slopes * convolve(cotangent, flipped(conv_out))
    gradient = (cotangent + convolve(backward, flipped(conv_in))).astype(jnp.bfloat16)
    lat_loc = band_matrix(LAT, False).astype(jnp.float32)
    lon_loc = band_matrix(LON, True).astype(jnp.float32)
    grad_wide = gradient.astype(jnp.float32)

    def member_step(carry, member):
        member_wide = member.astype(jnp.float32)
        product = (member_wide * grad_wide).astype(jnp.bfloat16).astype(jnp.float32)
        banded = jnp.einsum("xcy,yz->xcz", product, lat_loc, precision=lax.Precision.HIGHEST).astype(jnp.bfloat16).astype(jnp.float32)
        spread = jnp.einsum("zx,xcy->zcy", lon_loc, banded, precision=lax.Precision.HIGHEST)
        return carry + member_wide * spread, None

    start_sum = jnp.zeros(state.shape, jnp.float32)
    summed, unused = lax.scan(member_step, start_sum, members)
    increment = summed / (MEMBERS - 1.0)
    tangent_hidden = slopes * convolve(increment, conv_in)
    response = increment + convolve(tangent_hidden, conv_out)
    return increment, response
```

```python
import functools

import jax
import jax.numpy as jnp
from jax import lax
from jax.experimental import pallas as pl
from jax.experimental.pallas import tpu as pltpu
from jax.sharding import PartitionSpec as P

HALF = 16
LANES = 128


def flip(index, stride):
    return index + stride * (1 - 2 * lax.rem(index // stride, 2))


def flip_all(index, mask):
    stride = 1
    while stride <= mask:
        if mask & stride:
            index = flip(index, stride)
        stride *= 2
    return index


def stages_of(count):
    held = [0]
    steps = []
    stride = count // 2
    while stride >= 8:
        steps.append([(stride, list(held))])
        held = held + [m ^ stride for m in held]
        stride //= 2
    half = max(1, len(held) // 2)
    first, second = held[:half], held[half:]
    steps.append([(2, first), (4, second)])
    first = first + [m ^ 2 for m in first]
    second = second + [m ^ 4 for m in second]
    steps.append([(4, first), (2, second)])
    return steps


def greet(me, count, extra=()):
    barrier = pltpu.get_barrier_semaphore()
    friends = list(extra)
    stride = 1
    while stride < count:
        friends.append(flip(me, stride))
        stride *= 2
    for friend in friends:
        pl.semaphore_signal(
            barrier, inc=1, device_id={"space": friend}, device_id_type=pl.DeviceIdType.MESH
        )
    pl.semaphore_wait(barrier, len(friends))


def gather_kernel(count, block_ref, whole_ref, send_sem, recv_sem):
    me = lax.axis_index("space")
    greet(me, count)

    def remote(mask, stride):
        owner = flip_all(me, mask)
        source = block_ref if mask == 0 else whole_ref.at[owner]
        slot = mask ^ stride
        return pltpu.make_async_remote_copy(
            src_ref=source,
            dst_ref=whole_ref.at[owner],
            send_sem=send_sem.at[slot],
            recv_sem=recv_sem.at[slot],
            device_id={"space": flip(me, stride)},
            device_id_type=pl.DeviceIdType.MESH,
        )

    started = []
    pair = []
    for step in stages_of(count):
        now = []
        for position in range(max(len(masks) for stride, masks in step)):
            for stride, masks in step:
                if position < len(masks):
                    copy = remote(masks[position], stride)
                    copy.start()
                    now.append((copy, masks[position] ^ stride))
        if not pair:
            copy = remote(0, 1)
            copy.start()
            pair.append(copy)
            whole_ref[me] = block_ref[...]
        for copy, mask in now:
            copy.wait_recv()
            other = remote(mask, 1)
            other.start()
            pair.append(other)
            started.append(copy)
    for copy in started:
        copy.wait_send()
    for copy in pair:
        copy.wait()


def gather(block):
    count = lax.axis_size("space")
    return pl.pallas_call(
        functools.partial(gather_kernel, count),
        out_shape=jax.ShapeDtypeStruct((count,) + block.shape, block.dtype),
        in_specs=[pl.BlockSpec(memory_space=pltpu.VMEM)],
        out_specs=pl.BlockSpec(memory_space=pltpu.VMEM),
        scratch_shapes=[
            pltpu.SemaphoreType.DMA((count,)),
            pltpu.SemaphoreType.DMA((count,)),
        ],
        compiler_params=pltpu.CompilerParams(collective_id=0, has_side_effects=True),
        name="gather",
    )(block)


def scatter_kernel(
    count, rim, part_ref, sum_ref, left_ref, right_ref,
    out_buf, in_buf, edge_buf, send_sem, recv_sem, edge_send, edge_recv,
):
    me = lax.axis_index("space")
    before, after = lax.rem(me + count - 1, count), lax.rem(me + 1, count)
    greet(me, count, (before, after))
    arrived = {mask: [] for mask in range(count)}

    def value(mask):
        total = part_ref[flip_all(me, mask)]
        for slot in arrived[mask]:
            total = total + in_buf[slot].astype(jnp.float32)
        return total

    sent = []
    for step in [[(1, list(range(0, count, 2)))]] + stages_of(count)[::-1]:
        now = []
        for position in range(max(len(masks) for stride, masks in step)):
            for stride, masks in step:
                if position < len(masks):
                    slot = masks[position] ^ stride
                    out_buf[slot] = value(slot).astype(out_buf.dtype)
                    copy = pltpu.make_async_remote_copy(
                        src_ref=out_buf.at[slot],
                        dst_ref=in_buf.at[slot],
                        send_sem=send_sem.at[slot],
                        recv_sem=recv_sem.at[slot],
                        device_id={"space": flip(me, stride)},
                        device_id_type=pl.DeviceIdType.MESH,
                    )
                    copy.start()
                    now.append((copy, masks[position], slot))
        for copy, mask, slot in now:
            copy.wait_recv()
            arrived[mask].append(slot)
            sent.append(copy)
    total = value(0)
    sum_ref[...] = total
    edge_buf[0] = total[:rim]
    edge_buf[1] = total[total.shape[0] - rim :]
    edges = [
        pltpu.make_async_remote_copy(
            src_ref=edge_buf.at[side],
            dst_ref=target,
            send_sem=edge_send.at[side],
            recv_sem=edge_recv.at[side],
            device_id={"space": friend},
            device_id_type=pl.DeviceIdType.MESH,
        )
        for side, target, friend in ((0, right_ref, before), (1, left_ref, after))
    ]
    for copy in edges:
        copy.start()
    for copy in sent:
        copy.wait_send()
    for copy in edges:
        copy.wait()


def scatter(parts, rim):
    count, rows, lat_count = parts.shape
    return pl.pallas_call(
        functools.partial(scatter_kernel, count, rim),
        out_shape=(
            jax.ShapeDtypeStruct((rows, lat_count), jnp.float32),
            jax.ShapeDtypeStruct((rim, lat_count), jnp.float32),
            jax.ShapeDtypeStruct((rim, lat_count), jnp.float32),
        ),
        in_specs=[pl.BlockSpec(memory_space=pltpu.VMEM)],
        out_specs=(pl.BlockSpec(memory_space=pltpu.VMEM),) * 3,
        scratch_shapes=[
            pltpu.VMEM((count, rows, lat_count), jnp.bfloat16),
            pltpu.VMEM((count, rows, lat_count), jnp.bfloat16),
            pltpu.VMEM((2, rim, lat_count), jnp.float32),
            pltpu.SemaphoreType.DMA((count,)),
            pltpu.SemaphoreType.DMA((count,)),
            pltpu.SemaphoreType.DMA((2,)),
            pltpu.SemaphoreType.DMA((2,)),
        ],
        compiler_params=pltpu.CompilerParams(collective_id=1, has_side_effects=True),
        name="scatter",
    )(parts)


def covariance_kernel(members_ref, whole_ref, lat_ref, lon_ref, sum_ref, banded_ref):
    lat_count = lat_ref.shape[0]

    @pl.when(pl.program_id(0) == 0)
    def _():
        sum_ref[...] = jnp.zeros_like(sum_ref)

    for start in range(0, whole_ref.shape[1], lat_count):
        columns = slice(start, start + lat_count)
        product = members_ref[0, :, columns].astype(jnp.float32) * whole_ref[:, columns].astype(
            jnp.float32
        )
        banded_ref[:, columns] = jnp.dot(
            product.astype(jnp.bfloat16), lat_ref[...], preferred_element_type=jnp.float32
        ).astype(jnp.bfloat16)
    for start in range(0, whole_ref.shape[1], lat_count):
        columns = slice(start, start + lat_count)
        spread = jnp.dot(
            lon_ref[...], banded_ref[:, columns], preferred_element_type=jnp.float32
        )
        sum_ref[:, columns] += members_ref[0, :, columns].astype(jnp.float32) * spread


def covariance(members, whole, lat_loc, lon_loc):
    count, lon_count, width = members.shape
    return pl.pallas_call(
        covariance_kernel,
        grid=(count,),
        out_shape=jax.ShapeDtypeStruct((lon_count, width), jnp.float32),
        in_specs=[
            pl.BlockSpec((1, lon_count, width), lambda m: (m, 0, 0)),
            pl.BlockSpec(whole.shape, lambda m: (0, 0)),
            pl.BlockSpec(lat_loc.shape, lambda m: (0, 0)),
            pl.BlockSpec(lon_loc.shape, lambda m: (0, 0)),
        ],
        out_specs=pl.BlockSpec((lon_count, width), lambda m: (0, 0)),
        scratch_shapes=[pltpu.VMEM((lon_count, width), jnp.bfloat16)],
        name="covariance",
    )(members, whole, lat_loc, lon_loc)


def padded_2(cells, axis, width):
    count = lax.axis_size(axis)
    head = cells[:width]
    tail = cells[cells.shape[0] - width :]
    return jnp.concatenate(
        [
            lax.ppermute(tail, axis, [(i, (i + 1) % count) for i in range(count)]),
            cells,
            lax.ppermute(head, axis, [((i + 1) % count, i) for i in range(count)]),
        ],
        axis=0,
    )


def convolve(padded, weight, precision=None):
    row_count = padded.shape[0] - 2
    lat_count = padded.shape[2]
    out_count = weight.shape[2]
    in_count = weight.shape[3]
    if precision is None:
        padded = padded.astype(jnp.bfloat16)
        weight = weight.astype(jnp.bfloat16)
    if out_count <= in_count:
        flattened = weight.reshape(9 * out_count, in_count)
        product = jnp.einsum(
            "kc,xcy->xky", flattened, padded, preferred_element_type=jnp.float32
        )
        product = jnp.pad(product, ((0, 0), (0, 0), (1, 1)))
        summed = jnp.zeros((row_count, out_count, lat_count), jnp.float32)
        for step_lon in range(3):
            for step_lat in range(3):
                tap_index = step_lon * 3 + step_lat
                summed = (
                    summed
                    + product[
                        step_lon : step_lon + row_count,
                        tap_index * out_count : (tap_index + 1) * out_count,
                        step_lat : step_lat + lat_count,
                    ]
                )
        return summed
    lat_padded = jnp.pad(padded, ((0, 0), (0, 0), (1, 1)))
    stacked = jnp.concatenate(
        [
            lat_padded[step_lon : step_lon + row_count, :, step_lat : step_lat + lat_count]
            for step_lon in range(3)
            for step_lat in range(3)
        ],
        axis=1,
    )
    flattened = jnp.transpose(weight, (2, 0, 1, 3)).reshape(out_count, 9 * in_count)
    return jnp.einsum(
        "ok,xky->xoy", flattened, stacked, precision=precision, preferred_element_type=jnp.float32
    )


def split(values):
    high = lax.reduce_precision(values, 8, 7)
    return high.astype(jnp.bfloat16), (values - high).astype(jnp.bfloat16)


def convolve_fine(padded, weight):
    out_count, in_count = weight.shape[2:]
    upper, lower = split(padded)
    weight_upper, weight_lower = split(weight)
    if out_count <= in_count:
        both = jnp.concatenate([upper, lower], axis=1)
        stacked = jnp.concatenate([weight_upper, weight_lower], axis=2)
        stacked = jnp.concatenate([stacked, stacked], axis=3)
        result = convolve(both, stacked)
        return result[:, :out_count] + result[:, out_count:]
    return convolve(padded, weight, lax.Precision.HIGH)


def flipped(weight):
    return jnp.transpose(weight[::-1, ::-1], (0, 1, 3, 2))


def band_matrix(count, wrap):
    row_index = jnp.arange(count)[:, None]
    col_index = jnp.arange(count)[None, :]
    distance = jnp.abs(row_index - col_index)
    if wrap:
        distance = jnp.minimum(distance, count - distance)
    ratio = distance.astype(jnp.float32) / (HALF + 1.0)
    return jnp.where(distance <= HALF, 1.0 - ratio * ratio, 0.0).astype(jnp.bfloat16)


def tile_cols(t):
    return slice(t * LANES, (t + 1) * LANES)


def shifted(values, step):
    if step == 1:
        return values
    width = values.shape[-1]
    column = lax.broadcasted_iota(jnp.int32, values.shape, values.ndim - 1)
    if step == 0:
        return jnp.where(column == 0, 0.0, pltpu.roll(values, 1, values.ndim - 1))
    return jnp.where(column == width - 1, 0.0, pltpu.roll(values, width - 1, values.ndim - 1))


def tap_of(distance):
    ratio = distance / (HALF + 1.0)
    return jnp.where(distance <= HALF, 1.0 - ratio * ratio, 0.0)


def halves(values):
    high = values.astype(jnp.bfloat16)
    return high, (values - high.astype(jnp.float32)).astype(jnp.bfloat16)


def step_kernel(
    count, total_members,
    members_hbm, state_hbm, cot_hbm, win_hbm, wout_hbm, bias_hbm,
    incr_hbm, resp_hbm,
    mem_ref, own_ref, halo_ref, taps_ref, wraw_ref, bias_ref, slot_ref,
    w_state, w_cot, v_in, w_tail, v_tail,
    slopes_ref, part_ref, q_ref, g_ref, whole_ref, lat_ref, lon_ref, banded_ref, contrib_ref,
    out_buf, in_buf, total_ref, stage_ref,
    mem_sem, own_sem, small_sem, halo_send, halo_recv, g_send, g_recv, r_send, r_recv, out_sem,
):
    me = lax.axis_index("space")
    members, lane_tiles, lons, var_count, _ = mem_ref.shape
    rows = own_ref.shape[2]
    two = rows * var_count
    lats = lane_tiles * LANES
    hidden = slot_ref.shape[2]
    depth = count // 8
    before, after = lax.rem(me + count - 1, count), lax.rem(me + 1, count)

    own_loads = []
    for index, source in enumerate((state_hbm, cot_hbm)):
        for t in range(lane_tiles):
            copy = pltpu.make_async_copy(
                source.at[:, :, tile_cols(t)], own_ref.at[index, t], own_sem.at[index, t]
            )
            copy.start()
            own_loads.append(copy)
    small_loads = [
        pltpu.make_async_copy(win_hbm, wraw_ref.at[0], small_sem.at[0]),
        pltpu.make_async_copy(wout_hbm, wraw_ref.at[1], small_sem.at[1]),
        pltpu.make_async_copy(bias_hbm, bias_ref, small_sem.at[2]),
    ]
    for copy in small_loads:
        copy.start()
    mem_loads = []
    for m in range(members):
        for t in range(lane_tiles):
            copy = pltpu.make_async_copy(
                members_hbm.at[m, :, :, tile_cols(t)], mem_ref.at[m, t], mem_sem.at[m, t]
            )
            copy.start()
            mem_loads.append(copy)

    barrier = pltpu.get_barrier_semaphore()
    friends = [before, after] + [flip(me, 1), flip(me, 2), flip(me, 4)]
    friends += [flip_all(me, 8 * j) for j in range(1, depth)]
    for friend in friends:
        pl.semaphore_signal(
            barrier, inc=1, device_id={"space": friend}, device_id_type=pl.DeviceIdType.MESH
        )

    row = lax.broadcasted_iota(jnp.int32, taps_ref.shape[2:], 0)
    blank = jnp.where((row & 7) == 6, 1.0, 0.0)
    for index in range(2):
        for t in range(lane_tiles):
            taps_ref[index, t] = blank
    window = lat_ref.shape[1]
    for index in range(2):
        offset = index * (lats - window)
        y = lax.broadcasted_iota(jnp.int32, (window, window), 0)
        z = lax.broadcasted_iota(jnp.int32, (window, window), 1)
        value = tap_of(jnp.abs(y - z).astype(jnp.float32))
        mine = (z + offset < lats // 2) if index == 0 else (z + offset >= lats // 2)
        lat_ref[index] = jnp.where(mine, value, 0.0).astype(jnp.bfloat16)
    i = lax.broadcasted_iota(jnp.int32, lon_ref.shape, 0)
    j = lax.broadcasted_iota(jnp.int32, lon_ref.shape, 1)
    gap = i - j + var_count * HALF
    value = tap_of(jnp.abs(gap).astype(jnp.float32) * 0.5)
    lon_ref[...] = jnp.where((gap & 1) == 0, value, 0.0).astype(jnp.bfloat16)

    for copy in small_loads:
        copy.wait()
    slot_ref[...] = jnp.zeros(slot_ref.shape, jnp.float32)
    for a in range(3):
        for b in range(3):
            place = slice(8 * a + 2 * b, 8 * a + 2 * b + 2)
            slot_ref[0, place, :] = wraw_ref[0, a, b]
            slot_ref[1, place, :] = wraw_ref[0, 2 - a, 2 - b]
            slot_ref[2, place, :] = wraw_ref[1, 2 - a, 2 - b]
            slot_ref[3, place, :] = wraw_ref[1, a, b]
    w_tail[...] = slot_ref[0].T.astype(jnp.bfloat16)
    v_tail[...] = slot_ref[3].astype(jnp.bfloat16)
    slot_ref[0, 14:15, :] = bias_ref[...]
    for target, index in ((w_state, 0), (w_cot, 2)):
        high, low = halves(slot_ref[index].T)
        target[...] = jnp.concatenate([high, high, low], axis=1)
    high, low = halves(slot_ref[1])
    v_in[:32] = jnp.concatenate([high, high], axis=1)
    v_in[32:] = jnp.concatenate([low, low], axis=1)

    for copy in own_loads:
        copy.wait()
    pl.semaphore_wait(barrier, len(friends))
    edges = []
    for side, start, friend in ((1, 0, before), (0, rows - 2, after)):
        copy = pltpu.make_async_remote_copy(
            src_ref=own_ref.at[:, :, start : start + 2],
            dst_ref=halo_ref.at[side],
            send_sem=halo_send.at[side],
            recv_sem=halo_recv.at[side],
            device_id={"space": friend},
            device_id_type=pl.DeviceIdType.MESH,
        )
        copy.start()
        edges.append(copy)

    own_rows = own_ref.reshape(2, lane_tiles, two, LANES)
    for index in range(2):
        for c in range(var_count):
            values = jnp.concatenate(
                [own_rows[index, t, pl.ds(c, rows, stride=var_count), :] for t in range(lane_tiles)],
                axis=1,
            )
            for b in range(3):
                moved = shifted(values, b)
                for t in range(lane_tiles):
                    taps_ref[index, t, pl.ds(16 + 2 * b + c, rows, stride=8), :] = moved[:, tile_cols(t)]

    def lane_chunks():
        tiles = [(line, t) for line in range(2) for t in range(lane_tiles)]
        return [tiles[k : k + 2] for k in range(0, len(tiles), 2)]

    def tap_block(index, j, t):
        start = pl.multiple_of(8 * j, 8)
        return taps_ref[index, t, pl.ds(start, 32), :]

    def fine_block(index, j, t):
        high, low = halves(tap_block(index, j, t))
        return jnp.concatenate([high, low, high], axis=0)

    def head_pair(p):
        for chunk in lane_chunks():
            lines = [(2 * p + line, t) for line, t in chunk]
            field = jnp.concatenate([fine_block(0, j, t) for j, t in lines], axis=1)
            misfit = jnp.concatenate([fine_block(1, j, t) for j, t in lines], axis=1)
            activity = jnp.tanh(jnp.dot(w_state[...], field, preferred_element_type=jnp.float32))
            slopes = 1.0 - activity * activity
            back = slopes * jnp.dot(w_cot[...], misfit, preferred_element_type=jnp.float32)
            high, low = halves(back)
            pieces = jnp.dot(
                v_in[...], jnp.concatenate([high, low], axis=0), preferred_element_type=jnp.float32
            )
            pieces = pieces[:24] + pieces[32:56]
            for place, (j, t) in enumerate(lines):
                slopes_ref[j, :, tile_cols(t)] = slopes[:, tile_cols(place)]
                part_ref[j, :, tile_cols(t)] = pieces[:, tile_cols(place)]

    pairs = (rows + 2) // 2

    def inner(p, carry):
        head_pair(p)
        return carry

    lax.fori_loop(1, pairs - 1, inner, 0)

    for copy in edges:
        copy.wait()
    halo_rows = halo_ref.reshape(2, 2, lane_tiles, 2 * var_count, LANES)
    for side, slot in ((0, 0), (1, rows + 2)):
        for index in range(2):
            values = jnp.concatenate(
                [halo_rows[side, index, t] for t in range(lane_tiles)], axis=1
            )
            for b in range(3):
                moved = shifted(values, b)
                for line in range(2):
                    at = 8 * (slot + line) + 2 * b
                    for t in range(lane_tiles):
                        taps_ref[index, t, at : at + 2, :] = moved[
                            2 * line : 2 * line + 2, tile_cols(t)
                        ]

    def outer(p, carry):
        head_pair(p * (pairs - 1))
        return carry

    lax.fori_loop(0, 2, outer, 0)

    def assembled(c):
        return sum(
            shifted(tile_rows(q_ref, pl.ds(2 * b + c, rows, stride=8)), b) for b in range(3)
        )

    def tile_rows(ref, place):
        return jnp.concatenate([ref[t, place, :] for t in range(lane_tiles)], axis=1)

    def gather_pieces():
        for t in range(lane_tiles):
            cols = tile_cols(t)
            joined = (
                part_ref[0:rows, 0:8, cols]
                + part_ref[1 : rows + 1, 8:16, cols]
                + part_ref[2 : rows + 2, 16:24, cols]
            )
            q_ref[t] = joined.reshape(rows * 8, LANES)

    gather_pieces()
    for c in range(var_count):
        values = jnp.concatenate(
            [own_rows[1, t, pl.ds(c, rows, stride=var_count), :] for t in range(lane_tiles)], axis=1
        )
        values = values + assembled(c)
        for t in range(lane_tiles):
            g_ref[t, pl.ds(c, rows, stride=var_count), :] = values[:, tile_cols(t)]
    whole_ref[me] = tile_rows(g_ref, slice(None)).astype(jnp.bfloat16)

    forks = [j for j in range(depth) if bin(j).count("1") % 2 == 0]
    sends = []

    def pass_on(rel, stride):
        owner = flip_all(me, rel)
        slot = rel ^ stride
        copy = pltpu.make_async_remote_copy(
            src_ref=whole_ref.at[owner],
            dst_ref=whole_ref.at[owner],
            send_sem=g_send.at[len(sends)],
            recv_sem=g_recv.at[slot],
            device_id={"space": flip_all(me, stride)},
            device_id_type=pl.DeviceIdType.MESH,
        )
        copy.start()
        sends.append(copy)

    def await_block(rel):
        owner = flip_all(me, rel)
        pltpu.make_async_remote_copy(
            src_ref=whole_ref.at[owner],
            dst_ref=whole_ref.at[owner],
            send_sem=g_send.at[0],
            recv_sem=g_recv.at[rel],
            device_id={"space": flip(me, 1)},
            device_id_type=pl.DeviceIdType.MESH,
        ).wait_recv()

    pass_on(0, 2)
    pass_on(0, 4)
    for j in range(1, depth):
        pass_on(0, 8 * j)
    pass_on(0, 1)
    for j in range(depth):
        if j:
            await_block(8 * j)
            pass_on(8 * j, 2)
            pass_on(8 * j, 4)
            pass_on(8 * j, 1)
        if j == 0:
            for near in (2, 4):
                await_block(near)
                if (near == 4) == (j in forks):
                    pass_on(near, 6 - near)
                pass_on(near, 1)
    for j in range(1, depth):
        for near in (2, 4):
            rel = 8 * j + near
            await_block(rel)
            if (near == 4) == (j in forks):
                pass_on(rel, 6 - near)
            pass_on(rel, 1)
    for j in range(depth):
        await_block(8 * j + 6)
        pass_on(8 * j + 6, 1)
    for rel in range(1, count, 2):
        await_block(rel)
    for copy in mem_loads:
        copy.wait()
    mem_rows = mem_ref.reshape(members, lane_tiles, lons * var_count, LANES)
    margin = HALF * var_count

    def lat_step(d, carry):
        at = pl.multiple_of(d * two, 16)
        products = [
            [
                mem_rows[m, t, pl.ds(at, two), :] * whole_ref[d, :, tile_cols(t)]
                for t in range(lane_tiles)
            ]
            for m in range(members)
        ]
        sides = [
            jnp.dot(
                jnp.concatenate(
                    [jnp.concatenate(p[side : side + 2], axis=1) for p in products], axis=0
                ),
                lat_ref[side],
                preferred_element_type=jnp.float32,
            )
            for side in range(2)
        ]
        bands = [
            sides[0][:, :LANES],
            sides[0][:, LANES:] + sides[1][:, :LANES],
            sides[1][:, LANES:],
        ]
        for t, band in enumerate(bands):
            narrow = band.astype(jnp.bfloat16)
            for m in range(members):
                banded_ref[pl.ds(at + margin, two), tile_cols(t * members + m)] = narrow[
                    m * two : (m + 1) * two
                ]
        return carry

    lax.fori_loop(0, count, lat_step, 0)
    high_rows = lons * var_count
    banded_ref[:margin] = banded_ref[high_rows : high_rows + margin]
    banded_ref[high_rows + margin :] = banded_ref[margin : 2 * margin]

    band_rows, band_depth = lon_ref.shape

    def lon_step(q, carry):
        at = pl.multiple_of(q * band_rows, 16)
        for t in range(lane_tiles):
            total = jnp.zeros((band_rows, LANES), jnp.float32)
            for m in range(0, members, 2):
                start = (t * members + m) * LANES
                spread = jnp.dot(
                    lon_ref[...],
                    banded_ref[pl.ds(at, band_depth), start : start + 2 * LANES],
                    preferred_element_type=jnp.float32,
                )
                for k in range(2):
                    total += (
                        mem_rows[m + k, t, pl.ds(at, band_rows), :].astype(jnp.float32)
                        * spread[:, tile_cols(k)]
                    )
            contrib_ref[pl.ds(at + 8, band_rows), tile_cols(t)] = total
        return carry

    lax.fori_loop(0, high_rows // band_rows, lon_step, 0)
    contrib_ref[:8] = contrib_ref[high_rows : high_rows + 8]
    contrib_ref[high_rows + 8 :] = contrib_ref[8:16]

    for copy in sends:
        copy.wait_send()

    def part_of(rel):
        at = pl.multiple_of(flip_all(me, rel) * two, 16)
        body = contrib_ref[pl.ds(at + 8, two), :]
        ahead = contrib_ref[pl.ds(at, 8), :]
        behind = contrib_ref[pl.ds(at + 8 + two, 8), :]
        row = lax.broadcasted_iota(jnp.int32, (8, lats), 0)
        return body, jnp.where(row < 4, behind, ahead)

    reduce_sends = []

    def ship(value, slot, stride):
        out_buf[slot, :two] = value[0].astype(jnp.bfloat16)
        out_buf[slot, two:] = value[1].astype(jnp.bfloat16)
        copy = pltpu.make_async_remote_copy(
            src_ref=out_buf.at[slot],
            dst_ref=in_buf.at[slot],
            send_sem=r_send.at[slot],
            recv_sem=r_recv.at[slot],
            device_id={"space": flip_all(me, stride)},
            device_id_type=pl.DeviceIdType.MESH,
        )
        copy.start()
        reduce_sends.append(copy)
        return copy

    flying = {}

    def arrived(value, slot):
        flying[slot].wait_recv()
        return (
            value[0] + in_buf[slot, :two].astype(jnp.float32),
            value[1] + in_buf[slot, two:].astype(jnp.float32),
        )

    pair_slot = {}
    column_of = {6: 0, 2: 1, 4: 2, 0: 3}
    far = list(range(depth))[::-1]
    for column in (6, 2, 4, 0):
        for j in far:
            slot = column_of[column] * depth + j
            flying[slot] = ship(part_of(8 * j + column + 1), slot, 1)

    def chip_part(column, j):
        return arrived(part_of(8 * j + column), column_of[column] * depth + j)

    base = 4 * depth
    for j in far:
        slot = base + j
        flying[slot] = ship(chip_part(6, j), slot, 2 if j in forks else 4)
    for column in (2, 4):
        for j in far:
            if (column == 2) == (j in forks):
                slot = base + column // 2 * depth + j
                flying[slot] = ship(chip_part(column, j), slot, column)
    for j in far:
        column = 4 if j in forks else 2
        slot = base + column // 2 * depth + j
        value = arrived(chip_part(column, j), base + j)
        flying[slot] = ship(value, slot, column)
    last = base + 3 * depth
    value = None
    for j in far:
        value = chip_part(0, j)
        for column in (2, 4):
            value = arrived(value, base + column // 2 * depth + j)
        if j:
            flying[last + j] = ship(value, last + j, 8 * j)
    for j in range(1, depth):
        value = arrived(value, last + j)
    body = value[0] / (total_members - 1.0)
    rim = value[1] / (total_members - 1.0)
    stage_rows = stage_ref.reshape(2, lane_tiles, two, LANES)
    for t in range(lane_tiles):
        total_ref[t, 0:8, :] = rim[:, tile_cols(t)]
        total_ref[t, 8 : 8 + two, :] = body[:, tile_cols(t)]
        total_ref[t, 8 + two :, :] = rim[:, tile_cols(t)]
        stage_rows[0, t] = body[:, tile_cols(t)]
    stores = []

    def store(index, target):
        for t in range(lane_tiles):
            copy = pltpu.make_async_copy(
                stage_ref.at[index, t], target.at[:, :, tile_cols(t)], out_sem.at[index, t]
            )
            copy.start()
            stores.append(copy)

    store(0, incr_hbm)

    wide = rows + 4
    for c in range(var_count):
        values = tile_rows(total_ref, pl.ds(4 + c, wide, stride=var_count))
        for b in range(3):
            moved = shifted(values, b)
            for t in range(lane_tiles):
                taps_ref[0, t, pl.ds(2 * b + c, wide, stride=8), :] = moved[:, tile_cols(t)]

    def tail_pair(p, carry):
        for chunk in lane_chunks():
            lines = [(2 * p + line, t) for line, t in chunk]
            field = jnp.concatenate([tap_block(0, j, t) for j, t in lines], axis=1)
            tangent = jnp.dot(
                w_tail[...], field.astype(jnp.bfloat16), preferred_element_type=jnp.float32
            )
            slopes = jnp.concatenate([slopes_ref[j, :, tile_cols(t)] for j, t in lines], axis=1)
            pieces = jnp.dot(
                v_tail[...],
                (slopes * tangent).astype(jnp.bfloat16),
                preferred_element_type=jnp.float32,
            )
            for place, (j, t) in enumerate(lines):
                part_ref[j, :, tile_cols(t)] = pieces[:24, tile_cols(place)]
        return carry

    lax.fori_loop(0, pairs, tail_pair, 0)
    gather_pieces()
    for c in range(var_count):
        values = tile_rows(total_ref, pl.ds(8 + c, rows, stride=var_count)) + assembled(c)
        for t in range(lane_tiles):
            stage_rows[1, t, pl.ds(c, rows, stride=var_count), :] = values[:, tile_cols(t)]
    store(1, resp_hbm)
    for copy in stores:
        copy.wait()
    for copy in reduce_sends:
        copy.wait_send()


def whole_step(members, state, cotangent, conv_in, conv_out, bias):
    count = lax.axis_size("space")
    mine, lons, var_count, lats = members.shape
    rows = state.shape[0]
    hidden = bias.shape[0]
    two = rows * var_count
    tiles = lats // LANES
    depth = count // 8
    any_space = pl.BlockSpec(memory_space=pl.ANY)
    vmem = pltpu.VMEM
    dma = pltpu.SemaphoreType.DMA
    margin = HALF * var_count
    window = lats - LANES
    slots = 8 * depth
    return pl.pallas_call(
        functools.partial(step_kernel, count, mine * count),
        out_shape=(jax.ShapeDtypeStruct(state.shape, jnp.float32),) * 2,
        in_specs=[any_space] * 6,
        out_specs=(any_space,) * 2,
        scratch_shapes=[
            vmem((mine, tiles, lons, var_count, LANES), jnp.bfloat16),
            vmem((2, tiles, rows, var_count, LANES), jnp.float32),
            vmem((2, 2, tiles, 2, var_count, LANES), jnp.float32),
            vmem((2, tiles, (rows + 5) * 8, LANES), jnp.float32),
            vmem((2, 3, 3, var_count, hidden), jnp.float32),
            vmem((1, hidden), jnp.float32),
            vmem((4, 32, hidden), jnp.float32),
            vmem((hidden, 96), jnp.bfloat16),
            vmem((hidden, 96), jnp.bfloat16),
            vmem((64, 2 * hidden), jnp.bfloat16),
            vmem((hidden, 32), jnp.bfloat16),
            vmem((32, hidden), jnp.bfloat16),
            vmem((rows + 2, hidden, lats), jnp.float32),
            vmem((rows + 2, 24, lats), jnp.float32),
            vmem((tiles, rows * 8, LANES), jnp.float32),
            vmem((tiles, two, LANES), jnp.float32),
            vmem((count, two, lats), jnp.bfloat16),
            vmem((2, window, window), jnp.bfloat16),
            vmem((4 * two, 4 * two + 2 * margin), jnp.bfloat16),
            vmem((lons * var_count + 2 * margin, mine * lats), jnp.bfloat16),
            vmem((lons * var_count + 16, lats), jnp.float32),
            vmem((slots, two + 8, lats), jnp.bfloat16),
            vmem((slots, two + 8, lats), jnp.bfloat16),
            vmem((tiles, two + 16, LANES), jnp.float32),
            vmem((2, tiles, rows, var_count, LANES), jnp.float32),
            dma((mine, tiles)),
            dma((2, tiles)),
            dma((3,)),
            dma((2,)),
            dma((2,)),
            dma((count,)),
            dma((count,)),
            dma((slots,)),
            dma((slots,)),
            dma((2, tiles)),
        ],
        compiler_params=pltpu.CompilerParams(collective_id=2, has_side_effects=True),
        name="whole_step",
    )(
        members,
        state,
        cotangent,
        jnp.transpose(conv_in, (0, 1, 3, 2)),
        conv_out,
        bias.reshape(1, hidden),
    )


def fits(members, state, bias):
    count = lax.axis_size("space")
    mine, lons, var_count, lats = members.shape
    rows = state.shape[0]
    return (
        lax.axis_size("mem") == 1
        and count >= 8
        and count & (count - 1) == 0
        and var_count == 2
        and lats == 3 * LANES
        and rows % 8 == 0
        and rows >= 2 * 8
        and mine % 2 == 0
        and lons == count * rows
        and bias.shape[0] == LANES
    )


def per_device(members, state, cotangent, conv_in, conv_out, bias):
    row_count, var_count, lat_count = state.shape
    if fits(members, state, bias):
        return whole_step(members, state, cotangent, conv_in, conv_out, bias)
    count = lax.axis_size("space")
    direct = count >= 8 and count & (count - 1) == 0
    rim_width = 2
    joined = jnp.concatenate([state, cotangent], axis=1)
    padded = padded_2(joined, "space", rim_width)
    state_pad = padded[:, :var_count]
    cot_pad = padded[:, var_count:]
    activity = jnp.tanh(convolve_fine(state_pad, conv_in) + bias[None, :, None])
    slopes = 1.0 - activity * activity
    backward = slopes * convolve_fine(cot_pad, flipped(conv_out))
    gradient = cotangent + convolve_fine(backward, flipped(conv_in))
    gradient = gradient.astype(jnp.bfloat16)
    width = var_count * lat_count
    gradient = gradient.reshape(row_count, width)
    if direct:
        whole = gather(gradient).reshape(count * row_count, width)
    else:
        whole = lax.all_gather(gradient, "space", axis=0, tiled=True)
    merged = members.reshape(members.shape[0], members.shape[1], width)
    lat_loc = band_matrix(lat_count, False)
    lon_loc = band_matrix(merged.shape[1], True)
    contrib = covariance(merged, whole, lat_loc, lon_loc)
    member_count = members.shape[0] * lax.axis_size("space") * lax.axis_size("mem")
    if direct:
        own, left, right = scatter(
            contrib.reshape(count, row_count, width), rim_width
        )
        total = jnp.concatenate([left, own, right], axis=0)
        total = total.reshape(row_count + 2 * rim_width, var_count, lat_count)
        if lax.axis_size("mem") > 1:
            total = lax.psum(total, "mem")
        incr_pad = total / (member_count - 1.0)
        increment = incr_pad[rim_width : rim_width + row_count]
    else:
        member_sum = lax.psum(contrib, "mem")
        block_sum = lax.psum_scatter(member_sum, "space", scatter_dimension=0, tiled=True)
        increment = block_sum.reshape(state.shape) / (member_count - 1.0)
        incr_pad = padded_2(increment, "space", rim_width)
    tangent_hidden = slopes * convolve(incr_pad, conv_in)
    response = increment + convolve(tangent_hidden, conv_out)
    return (increment, response)


def solution(mesh):
    in_specs = (
        P(("space", "mem"), None, None, None),
        P("space", None, None),
        P("space", None, None),
        P(),
        P(),
        P(),
    )
    out_specs = (P("space", None, None), P("space", None, None))
    return jax.shard_map(
        per_device, mesh=mesh, in_specs=in_specs, out_specs=out_specs, check_vma=False
    )
```

```python
import functools

import jax
import jax.numpy as jnp
from jax import lax
from jax.experimental import pallas as pl
from jax.experimental.pallas import tpu as pltpu
from jax.sharding import PartitionSpec as P

HALF = 16
LANES = 128
HEAD_GROUP = 11
TAIL_GROUP = 13
LAT_GROUP = 8


def flip(index, stride):
    return index + stride * (1 - 2 * lax.rem(index // stride, 2))


def flip_all(index, mask):
    stride = 1
    while stride <= mask:
        if mask & stride:
            index = flip(index, stride)
        stride *= 2
    return index


def stages_of(count):
    held = [0]
    steps = []
    stride = count // 2
    while stride >= 8:
        steps.append([(stride, list(held))])
        held = held + [m ^ stride for m in held]
        stride //= 2
    half = max(1, len(held) // 2)
    first, second = held[:half], held[half:]
    steps.append([(2, first), (4, second)])
    first = first + [m ^ 2 for m in first]
    second = second + [m ^ 4 for m in second]
    steps.append([(4, first), (2, second)])
    return steps


def greet(me, count, extra=()):
    barrier = pltpu.get_barrier_semaphore()
    friends = list(extra)
    stride = 1
    while stride < count:
        friends.append(flip(me, stride))
        stride *= 2
    for friend in friends:
        pl.semaphore_signal(
            barrier, inc=1, device_id={"space": friend}, device_id_type=pl.DeviceIdType.MESH
        )
    pl.semaphore_wait(barrier, len(friends))


def gather_kernel(count, block_ref, whole_ref, send_sem, recv_sem):
    me = lax.axis_index("space")
    greet(me, count)

    def remote(mask, stride):
        owner = flip_all(me, mask)
        source = block_ref if mask == 0 else whole_ref.at[owner]
        slot = mask ^ stride
        return pltpu.make_async_remote_copy(
            src_ref=source,
            dst_ref=whole_ref.at[owner],
            send_sem=send_sem.at[slot],
            recv_sem=recv_sem.at[slot],
            device_id={"space": flip(me, stride)},
            device_id_type=pl.DeviceIdType.MESH,
        )

    started = []
    pair = []
    for step in stages_of(count):
        now = []
        for position in range(max(len(masks) for stride, masks in step)):
            for stride, masks in step:
                if position < len(masks):
                    copy = remote(masks[position], stride)
                    copy.start()
                    now.append((copy, masks[position] ^ stride))
        if not pair:
            copy = remote(0, 1)
            copy.start()
            pair.append(copy)
            whole_ref[me] = block_ref[...]
        for copy, mask in now:
            copy.wait_recv()
            other = remote(mask, 1)
            other.start()
            pair.append(other)
            started.append(copy)
    for copy in started:
        copy.wait_send()
    for copy in pair:
        copy.wait()


def gather(block):
    count = lax.axis_size("space")
    return pl.pallas_call(
        functools.partial(gather_kernel, count),
        out_shape=jax.ShapeDtypeStruct((count,) + block.shape, block.dtype),
        in_specs=[pl.BlockSpec(memory_space=pltpu.VMEM)],
        out_specs=pl.BlockSpec(memory_space=pltpu.VMEM),
        scratch_shapes=[
            pltpu.SemaphoreType.DMA((count,)),
            pltpu.SemaphoreType.DMA((count,)),
        ],
        compiler_params=pltpu.CompilerParams(collective_id=0, has_side_effects=True),
        name="gather",
    )(block)


def scatter_kernel(
    count, rim, part_ref, sum_ref, left_ref, right_ref,
    out_buf, in_buf, edge_buf, send_sem, recv_sem, edge_send, edge_recv,
):
    me = lax.axis_index("space")
    before, after = lax.rem(me + count - 1, count), lax.rem(me + 1, count)
    greet(me, count, (before, after))
    arrived = {mask: [] for mask in range(count)}

    def value(mask):
        total = part_ref[flip_all(me, mask)]
        for slot in arrived[mask]:
            total = total + in_buf[slot].astype(jnp.float32)
        return total

    sent = []
    for step in [[(1, list(range(0, count, 2)))]] + stages_of(count)[::-1]:
        now = []
        for position in range(max(len(masks) for stride, masks in step)):
            for stride, masks in step:
                if position < len(masks):
                    slot = masks[position] ^ stride
                    out_buf[slot] = value(slot).astype(out_buf.dtype)
                    copy = pltpu.make_async_remote_copy(
                        src_ref=out_buf.at[slot],
                        dst_ref=in_buf.at[slot],
                        send_sem=send_sem.at[slot],
                        recv_sem=recv_sem.at[slot],
                        device_id={"space": flip(me, stride)},
                        device_id_type=pl.DeviceIdType.MESH,
                    )
                    copy.start()
                    now.append((copy, masks[position], slot))
        for copy, mask, slot in now:
            copy.wait_recv()
            arrived[mask].append(slot)
            sent.append(copy)
    total = value(0)
    sum_ref[...] = total
    edge_buf[0] = total[:rim]
    edge_buf[1] = total[total.shape[0] - rim :]
    edges = [
        pltpu.make_async_remote_copy(
            src_ref=edge_buf.at[side],
            dst_ref=target,
            send_sem=edge_send.at[side],
            recv_sem=edge_recv.at[side],
            device_id={"space": friend},
            device_id_type=pl.DeviceIdType.MESH,
        )
        for side, target, friend in ((0, right_ref, before), (1, left_ref, after))
    ]
    for copy in edges:
        copy.start()
    for copy in sent:
        copy.wait_send()
    for copy in edges:
        copy.wait()


def scatter(parts, rim):
    count, rows, lat_count = parts.shape
    return pl.pallas_call(
        functools.partial(scatter_kernel, count, rim),
        out_shape=(
            jax.ShapeDtypeStruct((rows, lat_count), jnp.float32),
            jax.ShapeDtypeStruct((rim, lat_count), jnp.float32),
            jax.ShapeDtypeStruct((rim, lat_count), jnp.float32),
        ),
        in_specs=[pl.BlockSpec(memory_space=pltpu.VMEM)],
        out_specs=(pl.BlockSpec(memory_space=pltpu.VMEM),) * 3,
        scratch_shapes=[
            pltpu.VMEM((count, rows, lat_count), jnp.bfloat16),
            pltpu.VMEM((count, rows, lat_count), jnp.bfloat16),
            pltpu.VMEM((2, rim, lat_count), jnp.float32),
            pltpu.SemaphoreType.DMA((count,)),
            pltpu.SemaphoreType.DMA((count,)),
            pltpu.SemaphoreType.DMA((2,)),
            pltpu.SemaphoreType.DMA((2,)),
        ],
        compiler_params=pltpu.CompilerParams(collective_id=1, has_side_effects=True),
        name="scatter",
    )(parts)


def covariance_kernel(members_ref, whole_ref, lat_ref, lon_ref, sum_ref, banded_ref):
    lat_count = lat_ref.shape[0]

    @pl.when(pl.program_id(0) == 0)
    def _():
        sum_ref[...] = jnp.zeros_like(sum_ref)

    for start in range(0, whole_ref.shape[1], lat_count):
        columns = slice(start, start + lat_count)
        product = members_ref[0, :, columns].astype(jnp.float32) * whole_ref[:, columns].astype(
            jnp.float32
        )
        banded_ref[:, columns] = jnp.dot(
            product.astype(jnp.bfloat16), lat_ref[...], preferred_element_type=jnp.float32
        ).astype(jnp.bfloat16)
    for start in range(0, whole_ref.shape[1], lat_count):
        columns = slice(start, start + lat_count)
        spread = jnp.dot(
            lon_ref[...], banded_ref[:, columns], preferred_element_type=jnp.float32
        )
        sum_ref[:, columns] += members_ref[0, :, columns].astype(jnp.float32) * spread


def covariance(members, whole, lat_loc, lon_loc):
    count, lon_count, width = members.shape
    return pl.pallas_call(
        covariance_kernel,
        grid=(count,),
        out_shape=jax.ShapeDtypeStruct((lon_count, width), jnp.float32),
        in_specs=[
            pl.BlockSpec((1, lon_count, width), lambda m: (m, 0, 0)),
            pl.BlockSpec(whole.shape, lambda m: (0, 0)),
            pl.BlockSpec(lat_loc.shape, lambda m: (0, 0)),
            pl.BlockSpec(lon_loc.shape, lambda m: (0, 0)),
        ],
        out_specs=pl.BlockSpec((lon_count, width), lambda m: (0, 0)),
        scratch_shapes=[pltpu.VMEM((lon_count, width), jnp.bfloat16)],
        name="covariance",
    )(members, whole, lat_loc, lon_loc)


def padded_2(cells, axis, width):
    count = lax.axis_size(axis)
    head = cells[:width]
    tail = cells[cells.shape[0] - width :]
    return jnp.concatenate(
        [
            lax.ppermute(tail, axis, [(i, (i + 1) % count) for i in range(count)]),
            cells,
            lax.ppermute(head, axis, [((i + 1) % count, i) for i in range(count)]),
        ],
        axis=0,
    )


def convolve(padded, weight, precision=None):
    row_count = padded.shape[0] - 2
    lat_count = padded.shape[2]
    out_count = weight.shape[2]
    in_count = weight.shape[3]
    if precision is None:
        padded = padded.astype(jnp.bfloat16)
        weight = weight.astype(jnp.bfloat16)
    if out_count <= in_count:
        flattened = weight.reshape(9 * out_count, in_count)
        product = jnp.einsum(
            "kc,xcy->xky", flattened, padded, preferred_element_type=jnp.float32
        )
        product = jnp.pad(product, ((0, 0), (0, 0), (1, 1)))
        summed = jnp.zeros((row_count, out_count, lat_count), jnp.float32)
        for step_lon in range(3):
            for step_lat in range(3):
                tap_index = step_lon * 3 + step_lat
                summed = (
                    summed
                    + product[
                        step_lon : step_lon + row_count,
                        tap_index * out_count : (tap_index + 1) * out_count,
                        step_lat : step_lat + lat_count,
                    ]
                )
        return summed
    lat_padded = jnp.pad(padded, ((0, 0), (0, 0), (1, 1)))
    stacked = jnp.concatenate(
        [
            lat_padded[step_lon : step_lon + row_count, :, step_lat : step_lat + lat_count]
            for step_lon in range(3)
            for step_lat in range(3)
        ],
        axis=1,
    )
    flattened = jnp.transpose(weight, (2, 0, 1, 3)).reshape(out_count, 9 * in_count)
    return jnp.einsum(
        "ok,xky->xoy", flattened, stacked, precision=precision, preferred_element_type=jnp.float32
    )


def split(values):
    high = lax.reduce_precision(values, 8, 7)
    return high.astype(jnp.bfloat16), (values - high).astype(jnp.bfloat16)


def convolve_fine(padded, weight):
    out_count, in_count = weight.shape[2:]
    upper, lower = split(padded)
    weight_upper, weight_lower = split(weight)
    if out_count <= in_count:
        both = jnp.concatenate([upper, lower], axis=1)
        stacked = jnp.concatenate([weight_upper, weight_lower], axis=2)
        stacked = jnp.concatenate([stacked, stacked], axis=3)
        result = convolve(both, stacked)
        return result[:, :out_count] + result[:, out_count:]
    return convolve(padded, weight, lax.Precision.HIGH)


def flipped(weight):
    return jnp.transpose(weight[::-1, ::-1], (0, 1, 3, 2))


def band_matrix(count, wrap):
    row_index = jnp.arange(count)[:, None]
    col_index = jnp.arange(count)[None, :]
    distance = jnp.abs(row_index - col_index)
    if wrap:
        distance = jnp.minimum(distance, count - distance)
    ratio = distance.astype(jnp.float32) / (HALF + 1.0)
    return jnp.where(distance <= HALF, 1.0 - ratio * ratio, 0.0).astype(jnp.bfloat16)


def tile_cols(t):
    return slice(t * LANES, (t + 1) * LANES)


def shifted(values, step):
    if step == 1:
        return values
    width = values.shape[-1]
    column = lax.broadcasted_iota(jnp.int32, values.shape, values.ndim - 1)
    if step == 0:
        return jnp.where(column == 0, 0.0, pltpu.roll(values, 1, values.ndim - 1))
    return jnp.where(column == width - 1, 0.0, pltpu.roll(values, width - 1, values.ndim - 1))


def tap_of(distance):
    ratio = distance / (HALF + 1.0)
    return jnp.where(distance <= HALF, 1.0 - ratio * ratio, 0.0)


def halves(values):
    high = values.astype(jnp.bfloat16)
    return high, (values - high.astype(jnp.float32)).astype(jnp.bfloat16)


def step_kernel(
    count, total_members,
    members_hbm, state_hbm, cot_hbm, win_hbm, wout_hbm, bias_hbm,
    incr_hbm, resp_hbm,
    mem_ref, own_ref, halo_ref, taps_ref, wraw_ref, bias_ref, slot_ref,
    w_state, w_cot, v_in, w_tail, v_tail,
    slopes_ref, back_ref, part_ref, q_ref, g_ref, whole_ref, lat_ref, lon_ref, banded_ref, contrib_ref,
    out_buf, in_buf, total_ref, stage_ref,
    mem_sem, own_sem, small_sem, halo_send, halo_recv, g_send, g_recv, r_send, r_recv, out_sem,
):
    me = lax.axis_index("space")
    members, lane_tiles, high_rows, _ = mem_ref.shape
    var_count = wraw_ref.shape[3]
    two = own_ref.shape[2]
    rows = two // var_count
    lats = lane_tiles * LANES
    hidden = slot_ref.shape[2]
    depth = count // 8
    before, after = lax.rem(me + count - 1, count), lax.rem(me + 1, count)

    own_loads = []
    for index, source in enumerate((state_hbm, cot_hbm)):
        for t in range(lane_tiles):
            copy = pltpu.make_async_copy(
                source.reshape(two, lats).at[:, tile_cols(t)],
                own_ref.at[index, t],
                own_sem.at[index, t],
            )
            copy.start()
            own_loads.append(copy)
    small_loads = [
        pltpu.make_async_copy(win_hbm, wraw_ref.at[0], small_sem.at[0]),
        pltpu.make_async_copy(wout_hbm, wraw_ref.at[1], small_sem.at[1]),
        pltpu.make_async_copy(bias_hbm, bias_ref, small_sem.at[2]),
    ]
    for copy in small_loads:
        copy.start()
    mem_loads = []
    flat_members = members_hbm.reshape(members, high_rows, lats)
    for m in range(members):
        for t in range(lane_tiles):
            copy = pltpu.make_async_copy(
                flat_members.at[m, :, tile_cols(t)], mem_ref.at[m, t], mem_sem.at[m, t]
            )
            copy.start()
            mem_loads.append(copy)

    barrier = pltpu.get_barrier_semaphore()
    friends = [before, after] + [flip(me, 1), flip(me, 2), flip(me, 4)]
    friends += [flip_all(me, 8 * j) for j in range(1, depth)]
    for friend in friends:
        pl.semaphore_signal(
            barrier, inc=1, device_id={"space": friend}, device_id_type=pl.DeviceIdType.MESH
        )

    row = lax.broadcasted_iota(jnp.int32, taps_ref.shape[2:], 0)
    blank = jnp.where((row & 7) == 6, 1.0, 0.0)
    for index in range(2):
        for t in range(lane_tiles):
            taps_ref[index, t] = blank
    window = lat_ref.shape[1]
    for index in range(2):
        offset = index * (lats - window)
        y = lax.broadcasted_iota(jnp.int32, (window, window), 0)
        z = lax.broadcasted_iota(jnp.int32, (window, window), 1)
        value = tap_of(jnp.abs(y - z).astype(jnp.float32))
        mine = (z + offset < lats // 2) if index == 0 else (z + offset >= lats // 2)
        lat_ref[index] = jnp.where(mine, value, 0.0).astype(jnp.bfloat16)
    i = lax.broadcasted_iota(jnp.int32, lon_ref.shape, 0)
    j = lax.broadcasted_iota(jnp.int32, lon_ref.shape, 1)
    gap = i - j + var_count * HALF
    value = tap_of(jnp.abs(gap).astype(jnp.float32) * 0.5)
    lon_ref[...] = jnp.where((gap & 1) == 0, value, 0.0).astype(jnp.bfloat16)

    for copy in small_loads:
        copy.wait()
    slot_ref[...] = jnp.zeros(slot_ref.shape, jnp.float32)
    for a in range(3):
        for b in range(3):
            place = slice(8 * a + 2 * b, 8 * a + 2 * b + 2)
            slot_ref[0, place, :] = wraw_ref[0, a, b]
            slot_ref[1, place, :] = wraw_ref[0, 2 - a, 2 - b]
            slot_ref[2, place, :] = wraw_ref[1, 2 - a, 2 - b]
            slot_ref[3, place, :] = wraw_ref[1, a, b]
    w_tail[...] = slot_ref[0].T.astype(jnp.bfloat16)
    v_tail[...] = slot_ref[3].astype(jnp.bfloat16)
    slot_ref[0, 14:15, :] = bias_ref[...]
    for target, index in ((w_state, 0), (w_cot, 2)):
        high, low = halves(slot_ref[index].T)
        target[...] = jnp.concatenate([high, high, low], axis=1)
    high, low = halves(slot_ref[1])
    v_in[:32] = jnp.concatenate([high, high], axis=1)
    v_in[32:] = jnp.concatenate([low, low], axis=1)

    for copy in own_loads:
        copy.wait()
    pl.semaphore_wait(barrier, len(friends))
    edges = []
    for side, start, friend in ((1, 0, before), (0, two - 8, after)):
        copy = pltpu.make_async_remote_copy(
            src_ref=own_ref.at[:, :, start : start + 8],
            dst_ref=halo_ref.at[side],
            send_sem=halo_send.at[side],
            recv_sem=halo_recv.at[side],
            device_id={"space": friend},
            device_id_type=pl.DeviceIdType.MESH,
        )
        copy.start()
        edges.append(copy)

    for index in range(2):
        for c in range(var_count):
            values = jnp.concatenate(
                [own_ref[index, t, pl.ds(c, rows, stride=var_count), :] for t in range(lane_tiles)],
                axis=1,
            )
            for b in range(3):
                moved = shifted(values, b)
                for t in range(lane_tiles):
                    taps_ref[index, t, pl.ds(16 + 2 * b + c, rows, stride=8), :] = moved[:, tile_cols(t)]

    def lane_chunks():
        tiles = [(line, t) for line in range(2) for t in range(lane_tiles)]
        return [tiles[k : k + 2] for k in range(0, len(tiles), 2)]

    def tap_block(index, j, t):
        start = 8 * j if isinstance(j, int) else pl.multiple_of(8 * j, 8)
        return taps_ref[index, t, pl.ds(start, 32), :]

    def fine_block(index, j, t):
        high, low = halves(tap_block(index, j, t))
        return jnp.concatenate([high, low, high], axis=0)

    def in_groups(step, first, last, group):
        def several(k, carry):
            for place in range(group):
                step(first + k * group + place)
            return carry

        full = (last - first) // group
        lax.fori_loop(0, full, several, 0)
        for p in range(first + full * group, last):
            step(p)

    def head_pair(p):
        for chunk in lane_chunks():
            lines = [(2 * p + line, t) for line, t in chunk]
            field = jnp.concatenate([fine_block(0, j, t) for j, t in lines], axis=1)
            misfit = jnp.concatenate([fine_block(1, j, t) for j, t in lines], axis=1)
            activity = jnp.tanh(jnp.dot(w_state[...], field, preferred_element_type=jnp.float32))
            slopes = 1.0 - activity * activity
            back = slopes * jnp.dot(w_cot[...], misfit, preferred_element_type=jnp.float32)
            back = jnp.concatenate(halves(back), axis=0)
            for place, (j, t) in enumerate(lines):
                slopes_ref[j, :, tile_cols(t)] = slopes[:, tile_cols(place)]
                back_ref[j, :, tile_cols(t)] = back[:, tile_cols(place)]

    def project_pair(weights, p):
        for chunk in lane_chunks():
            lines = [(2 * p + line, t) for line, t in chunk]
            pieces = jnp.dot(
                weights,
                jnp.concatenate(
                    [back_ref[j, : weights.shape[1], tile_cols(t)] for j, t in lines], axis=1
                ),
                preferred_element_type=jnp.float32,
            )
            if pieces.shape[0] > 32:
                pieces = pieces[:32] + pieces[32:]
            for place, (j, t) in enumerate(lines):
                part_ref[j, :, tile_cols(t)] = pieces[:24, tile_cols(place)]

    pairs = (rows + 2) // 2

    in_groups(head_pair, 1, pairs - 1, HEAD_GROUP)
    in_groups(functools.partial(project_pair, v_in[...]), 1, pairs - 1, HEAD_GROUP)

    for copy in edges:
        copy.wait()
    for side, slot, first in ((0, 0, 4), (1, rows + 2, 0)):
        for index in range(2):
            values = jnp.concatenate(
                [halo_ref[side, index, t] for t in range(lane_tiles)], axis=1
            )
            for b in range(3):
                moved = shifted(values, b)
                for line in range(2):
                    at = 8 * (slot + line) + 2 * b
                    for t in range(lane_tiles):
                        taps_ref[index, t, at : at + 2, :] = moved[
                            first + 2 * line : first + 2 * line + 2, tile_cols(t)
                        ]

    for p in (0, pairs - 1):
        head_pair(p)
    for p in (0, pairs - 1):
        project_pair(v_in[...], p)

    def assembled(c):
        return sum(
            shifted(tile_rows(q_ref, pl.ds(2 * b + c, rows, stride=8)), b) for b in range(3)
        )

    def tile_rows(ref, place):
        return jnp.concatenate([ref[t, place, :] for t in range(lane_tiles)], axis=1)

    def gather_pieces():
        for t in range(lane_tiles):
            cols = tile_cols(t)
            joined = (
                part_ref[0:rows, 0:8, cols]
                + part_ref[1 : rows + 1, 8:16, cols]
                + part_ref[2 : rows + 2, 16:24, cols]
            )
            q_ref[t] = joined.reshape(rows * 8, LANES)

    gather_pieces()
    for c in range(var_count):
        values = jnp.concatenate(
            [own_ref[1, t, pl.ds(c, rows, stride=var_count), :] for t in range(lane_tiles)], axis=1
        )
        values = values + assembled(c)
        for t in range(lane_tiles):
            g_ref[t, pl.ds(c, rows, stride=var_count), :] = values[:, tile_cols(t)]
    whole_ref[me] = tile_rows(g_ref, slice(None)).astype(jnp.bfloat16)

    forks = [j for j in range(depth) if bin(j).count("1") % 2 == 0]
    sends = []

    def pass_on(rel, stride):
        owner = flip_all(me, rel)
        slot = rel ^ stride
        copy = pltpu.make_async_remote_copy(
            src_ref=whole_ref.at[owner],
            dst_ref=whole_ref.at[owner],
            send_sem=g_send.at[len(sends)],
            recv_sem=g_recv.at[slot],
            device_id={"space": flip_all(me, stride)},
            device_id_type=pl.DeviceIdType.MESH,
        )
        copy.start()
        sends.append(copy)

    def await_block(rel):
        owner = flip_all(me, rel)
        pltpu.make_async_remote_copy(
            src_ref=whole_ref.at[owner],
            dst_ref=whole_ref.at[owner],
            send_sem=g_send.at[0],
            recv_sem=g_recv.at[rel],
            device_id={"space": flip(me, 1)},
            device_id_type=pl.DeviceIdType.MESH,
        ).wait_recv()

    pass_on(0, 2)
    pass_on(0, 4)
    for j in range(1, depth):
        pass_on(0, 8 * j)
    pass_on(0, 1)
    for j in range(depth):
        if j:
            await_block(8 * j)
            pass_on(8 * j, 2)
            pass_on(8 * j, 4)
            pass_on(8 * j, 1)
        if j == 0:
            for near in (2, 4):
                await_block(near)
                if (near == 4) == (j in forks):
                    pass_on(near, 6 - near)
                pass_on(near, 1)
    for j in range(1, depth):
        for near in (2, 4):
            rel = 8 * j + near
            await_block(rel)
            if (near == 4) == (j in forks):
                pass_on(rel, 6 - near)
            pass_on(rel, 1)
    for j in range(depth):
        await_block(8 * j + 6)
        pass_on(8 * j + 6, 1)
    for rel in range(1, count, 2):
        await_block(rel)
    for copy in mem_loads:
        copy.wait()
    margin = HALF * var_count

    span = LAT_GROUP * two

    def lat_step(d, carry):
        at = pl.multiple_of(d * span, 16)
        fields = [
            whole_ref[pl.ds(d * LAT_GROUP, LAT_GROUP), :, tile_cols(t)].reshape(span, LANES)
            for t in range(lane_tiles)
        ]
        products = [
            [mem_ref[m, t, pl.ds(at, span), :] * fields[t] for t in range(lane_tiles)]
            for m in range(members)
        ]
        sides = [
            jnp.dot(
                jnp.concatenate(
                    [jnp.concatenate(p[side : side + 2], axis=1) for p in products], axis=0
                ),
                lat_ref[side],
                preferred_element_type=jnp.float32,
            )
            for side in range(2)
        ]
        bands = [
            sides[0][:, :LANES],
            sides[0][:, LANES:] + sides[1][:, :LANES],
            sides[1][:, LANES:],
        ]
        for t, band in enumerate(bands):
            narrow = band.astype(jnp.bfloat16)
            for m in range(members):
                banded_ref[pl.ds(at + margin, span), tile_cols(t * members + m)] = narrow[
                    m * span : (m + 1) * span
                ]
        return carry

    lax.fori_loop(0, count // LAT_GROUP, lat_step, 0)
    banded_ref[:margin] = banded_ref[high_rows : high_rows + margin]
    banded_ref[high_rows + margin :] = banded_ref[margin : 2 * margin]

    band_rows, band_depth = lon_ref.shape

    def lon_step(q, carry):
        at = pl.multiple_of(q * band_rows, 16)
        for t in range(lane_tiles):
            total = jnp.zeros((band_rows, LANES), jnp.float32)
            for m in range(0, members, 2):
                start = (t * members + m) * LANES
                spread = jnp.dot(
                    lon_ref[...],
                    banded_ref[pl.ds(at, band_depth), start : start + 2 * LANES],
                    preferred_element_type=jnp.float32,
                )
                for k in range(2):
                    total += (
                        mem_ref[m + k, t, pl.ds(at, band_rows), :].astype(jnp.float32)
                        * spread[:, tile_cols(k)]
                    )
            contrib_ref[pl.ds(at + 8, band_rows), tile_cols(t)] = total
        return carry

    lax.fori_loop(0, high_rows // band_rows, lon_step, 0)
    contrib_ref[:8] = contrib_ref[high_rows : high_rows + 8]
    contrib_ref[high_rows + 8 :] = contrib_ref[8:16]

    for copy in sends:
        copy.wait_send()

    def part_of(rel):
        at = pl.multiple_of(flip_all(me, rel) * two, 16)
        body = contrib_ref[pl.ds(at + 8, two), :]
        ahead = contrib_ref[pl.ds(at, 8), :]
        behind = contrib_ref[pl.ds(at + 8 + two, 8), :]
        row = lax.broadcasted_iota(jnp.int32, (8, lats), 0)
        return body, jnp.where(row < 4, behind, ahead)

    reduce_sends = []

    def ship(value, slot, stride):
        out_buf[slot, :two] = value[0].astype(jnp.bfloat16)
        out_buf[slot, two:] = value[1].astype(jnp.bfloat16)
        copy = pltpu.make_async_remote_copy(
            src_ref=out_buf.at[slot],
            dst_ref=in_buf.at[slot],
            send_sem=r_send.at[slot],
            recv_sem=r_recv.at[slot],
            device_id={"space": flip_all(me, stride)},
            device_id_type=pl.DeviceIdType.MESH,
        )
        copy.start()
        reduce_sends.append(copy)
        return copy

    flying = {}

    def arrived(value, slot):
        flying[slot].wait_recv()
        return (
            value[0] + in_buf[slot, :two].astype(jnp.float32),
            value[1] + in_buf[slot, two:].astype(jnp.float32),
        )

    pair_slot = {}
    column_of = {6: 0, 2: 1, 4: 2, 0: 3}
    far = list(range(depth))[::-1]
    for column in (6, 2, 4, 0):
        for j in far:
            slot = column_of[column] * depth + j
            flying[slot] = ship(part_of(8 * j + column + 1), slot, 1)

    def chip_part(column, j):
        return arrived(part_of(8 * j + column), column_of[column] * depth + j)

    base = 4 * depth
    for j in far:
        slot = base + j
        flying[slot] = ship(chip_part(6, j), slot, 2 if j in forks else 4)
    for column in (2, 4):
        for j in far:
            if (column == 2) == (j in forks):
                slot = base + column // 2 * depth + j
                flying[slot] = ship(chip_part(column, j), slot, column)
    for j in far:
        column = 4 if j in forks else 2
        slot = base + column // 2 * depth + j
        value = arrived(chip_part(column, j), base + j)
        flying[slot] = ship(value, slot, column)
    last = base + 3 * depth
    value = None
    for j in far:
        value = chip_part(0, j)
        for column in (2, 4):
            value = arrived(value, base + column // 2 * depth + j)
        if j:
            flying[last + j] = ship(value, last + j, 8 * j)
    for j in range(1, depth):
        value = arrived(value, last + j)
    body = value[0] / (total_members - 1.0)
    rim = value[1] / (total_members - 1.0)
    for t in range(lane_tiles):
        total_ref[t, 0:8, :] = rim[:, tile_cols(t)]
        total_ref[t, 8 : 8 + two, :] = body[:, tile_cols(t)]
        total_ref[t, 8 + two :, :] = rim[:, tile_cols(t)]
        stage_ref[0, t] = body[:, tile_cols(t)]
    stores = []

    def store(index, target):
        for t in range(lane_tiles):
            copy = pltpu.make_async_copy(
                stage_ref.at[index, t],
                target.reshape(two, lats).at[:, tile_cols(t)],
                out_sem.at[index, t],
            )
            copy.start()
            stores.append(copy)

    store(0, incr_hbm)

    wide = rows + 4
    for c in range(var_count):
        values = tile_rows(total_ref, pl.ds(4 + c, wide, stride=var_count))
        for b in range(3):
            moved = shifted(values, b)
            for t in range(lane_tiles):
                taps_ref[0, t, pl.ds(2 * b + c, wide, stride=8), :] = moved[:, tile_cols(t)]

    def tail_pair(p):
        for chunk in lane_chunks():
            lines = [(2 * p + line, t) for line, t in chunk]
            field = jnp.concatenate([tap_block(0, j, t) for j, t in lines], axis=1)
            tangent = jnp.dot(
                w_tail[...], field.astype(jnp.bfloat16), preferred_element_type=jnp.float32
            )
            slopes = jnp.concatenate([slopes_ref[j, :, tile_cols(t)] for j, t in lines], axis=1)
            back = (slopes * tangent).astype(jnp.bfloat16)
            for place, (j, t) in enumerate(lines):
                back_ref[j, :hidden, tile_cols(t)] = back[:, tile_cols(place)]

    in_groups(tail_pair, 0, pairs, TAIL_GROUP)
    in_groups(functools.partial(project_pair, v_tail[...]), 0, pairs, TAIL_GROUP)
    gather_pieces()
    for c in range(var_count):
        values = tile_rows(total_ref, pl.ds(8 + c, rows, stride=var_count)) + assembled(c)
        for t in range(lane_tiles):
            stage_ref[1, t, pl.ds(c, rows, stride=var_count), :] = values[:, tile_cols(t)]
    store(1, resp_hbm)
    for copy in stores:
        copy.wait()
    for copy in reduce_sends:
        copy.wait_send()


def whole_step(members, state, cotangent, conv_in, conv_out, bias):
    count = lax.axis_size("space")
    mine, lons, var_count, lats = members.shape
    rows = state.shape[0]
    hidden = bias.shape[0]
    two = rows * var_count
    tiles = lats // LANES
    depth = count // 8
    any_space = pl.BlockSpec(memory_space=pl.ANY)
    vmem = pltpu.VMEM
    dma = pltpu.SemaphoreType.DMA
    margin = HALF * var_count
    window = lats - LANES
    slots = 8 * depth
    return pl.pallas_call(
        functools.partial(step_kernel, count, mine * count),
        out_shape=(jax.ShapeDtypeStruct(state.shape, jnp.float32),) * 2,
        in_specs=[any_space] * 6,
        out_specs=(any_space,) * 2,
        scratch_shapes=[
            vmem((mine, tiles, lons * var_count, LANES), jnp.bfloat16),
            vmem((2, tiles, two, LANES), jnp.float32),
            vmem((2, 2, tiles, 8, LANES), jnp.float32),
            vmem((2, tiles, (rows + 5) * 8, LANES), jnp.float32),
            vmem((2, 3, 3, var_count, hidden), jnp.float32),
            vmem((1, hidden), jnp.float32),
            vmem((4, 32, hidden), jnp.float32),
            vmem((hidden, 96), jnp.bfloat16),
            vmem((hidden, 96), jnp.bfloat16),
            vmem((64, 2 * hidden), jnp.bfloat16),
            vmem((hidden, 32), jnp.bfloat16),
            vmem((32, hidden), jnp.bfloat16),
            vmem((rows + 2, hidden, lats), jnp.float32),
            vmem((rows + 2, 2 * hidden, lats), jnp.bfloat16),
            vmem((rows + 2, 24, lats), jnp.float32),
            vmem((tiles, rows * 8, LANES), jnp.float32),
            vmem((tiles, two, LANES), jnp.float32),
            vmem((count, two, lats), jnp.bfloat16),
            vmem((2, window, window), jnp.bfloat16),
            vmem((4 * two, 4 * two + 2 * margin), jnp.bfloat16),
            vmem((lons * var_count + 2 * margin, mine * lats), jnp.bfloat16),
            vmem((lons * var_count + 16, lats), jnp.float32),
            vmem((slots, two + 8, lats), jnp.bfloat16),
            vmem((slots, two + 8, lats), jnp.bfloat16),
            vmem((tiles, two + 16, LANES), jnp.float32),
            vmem((2, tiles, two, LANES), jnp.float32),
            dma((mine, tiles)),
            dma((2, tiles)),
            dma((3,)),
            dma((2,)),
            dma((2,)),
            dma((count,)),
            dma((count,)),
            dma((slots,)),
            dma((slots,)),
            dma((2, tiles)),
        ],
        compiler_params=pltpu.CompilerParams(collective_id=2, has_side_effects=True),
        name="whole_step",
    )(
        members,
        state,
        cotangent,
        jnp.transpose(conv_in, (0, 1, 3, 2)),
        conv_out,
        bias.reshape(1, hidden),
    )


def fits(members, state, bias):
    count = lax.axis_size("space")
    mine, lons, var_count, lats = members.shape
    rows = state.shape[0]
    return (
        lax.axis_size("mem") == 1
        and count >= 8
        and count & (count - 1) == 0
        and var_count == 2
        and lats == 3 * LANES
        and rows % 8 == 0
        and rows >= 2 * 8
        and mine % 2 == 0
        and lons == count * rows
        and bias.shape[0] == LANES
    )


def per_device(members, state, cotangent, conv_in, conv_out, bias):
    row_count, var_count, lat_count = state.shape
    if fits(members, state, bias):
        return whole_step(members, state, cotangent, conv_in, conv_out, bias)
    count = lax.axis_size("space")
    direct = count >= 8 and count & (count - 1) == 0
    rim_width = 2
    joined = jnp.concatenate([state, cotangent], axis=1)
    padded = padded_2(joined, "space", rim_width)
    state_pad = padded[:, :var_count]
    cot_pad = padded[:, var_count:]
    activity = jnp.tanh(convolve_fine(state_pad, conv_in) + bias[None, :, None])
    slopes = 1.0 - activity * activity
    backward = slopes * convolve_fine(cot_pad, flipped(conv_out))
    gradient = cotangent + convolve_fine(backward, flipped(conv_in))
    gradient = gradient.astype(jnp.bfloat16)
    width = var_count * lat_count
    gradient = gradient.reshape(row_count, width)
    if direct:
        whole = gather(gradient).reshape(count * row_count, width)
    else:
        whole = lax.all_gather(gradient, "space", axis=0, tiled=True)
    merged = members.reshape(members.shape[0], members.shape[1], width)
    lat_loc = band_matrix(lat_count, False)
    lon_loc = band_matrix(merged.shape[1], True)
    contrib = covariance(merged, whole, lat_loc, lon_loc)
    member_count = members.shape[0] * lax.axis_size("space") * lax.axis_size("mem")
    if direct:
        own, left, right = scatter(
            contrib.reshape(count, row_count, width), rim_width
        )
        total = jnp.concatenate([left, own, right], axis=0)
        total = total.reshape(row_count + 2 * rim_width, var_count, lat_count)
        if lax.axis_size("mem") > 1:
            total = lax.psum(total, "mem")
        incr_pad = total / (member_count - 1.0)
        increment = incr_pad[rim_width : rim_width + row_count]
    else:
        member_sum = lax.psum(contrib, "mem")
        block_sum = lax.psum_scatter(member_sum, "space", scatter_dimension=0, tiled=True)
        increment = block_sum.reshape(state.shape) / (member_count - 1.0)
        incr_pad = padded_2(increment, "space", rim_width)
    tangent_hidden = slopes * convolve(incr_pad, conv_in)
    response = increment + convolve(tangent_hidden, conv_out)
    return (increment, response)


def solution(mesh):
    in_specs = (
        P(("space", "mem"), None, None, None),
        P("space", None, None),
        P("space", None, None),
        P(),
        P(),
        P(),
    )
    out_specs = (P("space", None, None), P("space", None, None))
    return jax.shard_map(
        per_device, mesh=mesh, in_specs=in_specs, out_specs=out_specs, check_vma=False
    )
```

```python
import functools

import jax
import jax.numpy as jnp
from jax import lax
from jax.experimental import pallas as pl
from jax.experimental.pallas import tpu as pltpu
from jax.sharding import PartitionSpec as P

HALF = 16
LANES = 128
HEAD_GROUP = 11
TAIL_GROUP = 13


def flip(index, stride):
    return index + stride * (1 - 2 * lax.rem(index // stride, 2))


def flip_all(index, mask):
    stride = 1
    while stride <= mask:
        if mask & stride:
            index = flip(index, stride)
        stride *= 2
    return index


def stages_of(count):
    held = [0]
    steps = []
    stride = count // 2
    while stride >= 8:
        steps.append([(stride, list(held))])
        held = held + [m ^ stride for m in held]
        stride //= 2
    half = max(1, len(held) // 2)
    first, second = held[:half], held[half:]
    steps.append([(2, first), (4, second)])
    first = first + [m ^ 2 for m in first]
    second = second + [m ^ 4 for m in second]
    steps.append([(4, first), (2, second)])
    return steps


def greet(me, count, extra=()):
    barrier = pltpu.get_barrier_semaphore()
    friends = list(extra)
    stride = 1
    while stride < count:
        friends.append(flip(me, stride))
        stride *= 2
    for friend in friends:
        pl.semaphore_signal(
            barrier, inc=1, device_id={"space": friend}, device_id_type=pl.DeviceIdType.MESH
        )
    pl.semaphore_wait(barrier, len(friends))


def gather_kernel(count, block_ref, whole_ref, send_sem, recv_sem):
    me = lax.axis_index("space")
    greet(me, count)

    def remote(mask, stride):
        owner = flip_all(me, mask)
        source = block_ref if mask == 0 else whole_ref.at[owner]
        slot = mask ^ stride
        return pltpu.make_async_remote_copy(
            src_ref=source,
            dst_ref=whole_ref.at[owner],
            send_sem=send_sem.at[slot],
            recv_sem=recv_sem.at[slot],
            device_id={"space": flip(me, stride)},
            device_id_type=pl.DeviceIdType.MESH,
        )

    started = []
    pair = []
    for step in stages_of(count):
        now = []
        for position in range(max(len(masks) for stride, masks in step)):
            for stride, masks in step:
                if position < len(masks):
                    copy = remote(masks[position], stride)
                    copy.start()
                    now.append((copy, masks[position] ^ stride))
        if not pair:
            copy = remote(0, 1)
            copy.start()
            pair.append(copy)
            whole_ref[me] = block_ref[...]
        for copy, mask in now:
            copy.wait_recv()
            other = remote(mask, 1)
            other.start()
            pair.append(other)
            started.append(copy)
    for copy in started:
        copy.wait_send()
    for copy in pair:
        copy.wait()


def gather(block):
    count = lax.axis_size("space")
    return pl.pallas_call(
        functools.partial(gather_kernel, count),
        out_shape=jax.ShapeDtypeStruct((count,) + block.shape, block.dtype),
        in_specs=[pl.BlockSpec(memory_space=pltpu.VMEM)],
        out_specs=pl.BlockSpec(memory_space=pltpu.VMEM),
        scratch_shapes=[
            pltpu.SemaphoreType.DMA((count,)),
            pltpu.SemaphoreType.DMA((count,)),
        ],
        compiler_params=pltpu.CompilerParams(collective_id=0, has_side_effects=True),
        name="gather",
    )(block)


def scatter_kernel(
    count, rim, part_ref, sum_ref, left_ref, right_ref,
    out_buf, in_buf, edge_buf, send_sem, recv_sem, edge_send, edge_recv,
):
    me = lax.axis_index("space")
    before, after = lax.rem(me + count - 1, count), lax.rem(me + 1, count)
    greet(me, count, (before, after))
    arrived = {mask: [] for mask in range(count)}

    def value(mask):
        total = part_ref[flip_all(me, mask)]
        for slot in arrived[mask]:
            total = total + in_buf[slot].astype(jnp.float32)
        return total

    sent = []
    for step in [[(1, list(range(0, count, 2)))]] + stages_of(count)[::-1]:
        now = []
        for position in range(max(len(masks) for stride, masks in step)):
            for stride, masks in step:
                if position < len(masks):
                    slot = masks[position] ^ stride
                    out_buf[slot] = value(slot).astype(out_buf.dtype)
                    copy = pltpu.make_async_remote_copy(
                        src_ref=out_buf.at[slot],
                        dst_ref=in_buf.at[slot],
                        send_sem=send_sem.at[slot],
                        recv_sem=recv_sem.at[slot],
                        device_id={"space": flip(me, stride)},
                        device_id_type=pl.DeviceIdType.MESH,
                    )
                    copy.start()
                    now.append((copy, masks[position], slot))
        for copy, mask, slot in now:
            copy.wait_recv()
            arrived[mask].append(slot)
            sent.append(copy)
    total = value(0)
    sum_ref[...] = total
    edge_buf[0] = total[:rim]
    edge_buf[1] = total[total.shape[0] - rim :]
    edges = [
        pltpu.make_async_remote_copy(
            src_ref=edge_buf.at[side],
            dst_ref=target,
            send_sem=edge_send.at[side],
            recv_sem=edge_recv.at[side],
            device_id={"space": friend},
            device_id_type=pl.DeviceIdType.MESH,
        )
        for side, target, friend in ((0, right_ref, before), (1, left_ref, after))
    ]
    for copy in edges:
        copy.start()
    for copy in sent:
        copy.wait_send()
    for copy in edges:
        copy.wait()


def scatter(parts, rim):
    count, rows, lat_count = parts.shape
    return pl.pallas_call(
        functools.partial(scatter_kernel, count, rim),
        out_shape=(
            jax.ShapeDtypeStruct((rows, lat_count), jnp.float32),
            jax.ShapeDtypeStruct((rim, lat_count), jnp.float32),
            jax.ShapeDtypeStruct((rim, lat_count), jnp.float32),
        ),
        in_specs=[pl.BlockSpec(memory_space=pltpu.VMEM)],
        out_specs=(pl.BlockSpec(memory_space=pltpu.VMEM),) * 3,
        scratch_shapes=[
            pltpu.VMEM((count, rows, lat_count), jnp.bfloat16),
            pltpu.VMEM((count, rows, lat_count), jnp.bfloat16),
            pltpu.VMEM((2, rim, lat_count), jnp.float32),
            pltpu.SemaphoreType.DMA((count,)),
            pltpu.SemaphoreType.DMA((count,)),
            pltpu.SemaphoreType.DMA((2,)),
            pltpu.SemaphoreType.DMA((2,)),
        ],
        compiler_params=pltpu.CompilerParams(collective_id=1, has_side_effects=True),
        name="scatter",
    )(parts)


def covariance_kernel(members_ref, whole_ref, lat_ref, lon_ref, sum_ref, banded_ref):
    lat_count = lat_ref.shape[0]

    @pl.when(pl.program_id(0) == 0)
    def _():
        sum_ref[...] = jnp.zeros_like(sum_ref)

    for start in range(0, whole_ref.shape[1], lat_count):
        columns = slice(start, start + lat_count)
        product = members_ref[0, :, columns].astype(jnp.float32) * whole_ref[:, columns].astype(
            jnp.float32
        )
        banded_ref[:, columns] = jnp.dot(
            product.astype(jnp.bfloat16), lat_ref[...], preferred_element_type=jnp.float32
        ).astype(jnp.bfloat16)
    for start in range(0, whole_ref.shape[1], lat_count):
        columns = slice(start, start + lat_count)
        spread = jnp.dot(
            lon_ref[...], banded_ref[:, columns], preferred_element_type=jnp.float32
        )
        sum_ref[:, columns] += members_ref[0, :, columns].astype(jnp.float32) * spread


def covariance(members, whole, lat_loc, lon_loc):
    count, lon_count, width = members.shape
    return pl.pallas_call(
        covariance_kernel,
        grid=(count,),
        out_shape=jax.ShapeDtypeStruct((lon_count, width), jnp.float32),
        in_specs=[
            pl.BlockSpec((1, lon_count, width), lambda m: (m, 0, 0)),
            pl.BlockSpec(whole.shape, lambda m: (0, 0)),
            pl.BlockSpec(lat_loc.shape, lambda m: (0, 0)),
            pl.BlockSpec(lon_loc.shape, lambda m: (0, 0)),
        ],
        out_specs=pl.BlockSpec((lon_count, width), lambda m: (0, 0)),
        scratch_shapes=[pltpu.VMEM((lon_count, width), jnp.bfloat16)],
        name="covariance",
    )(members, whole, lat_loc, lon_loc)


def padded_2(cells, axis, width):
    count = lax.axis_size(axis)
    head = cells[:width]
    tail = cells[cells.shape[0] - width :]
    return jnp.concatenate(
        [
            lax.ppermute(tail, axis, [(i, (i + 1) % count) for i in range(count)]),
            cells,
            lax.ppermute(head, axis, [((i + 1) % count, i) for i in range(count)]),
        ],
        axis=0,
    )


def convolve(padded, weight, precision=None):
    row_count = padded.shape[0] - 2
    lat_count = padded.shape[2]
    out_count = weight.shape[2]
    in_count = weight.shape[3]
    if precision is None:
        padded = padded.astype(jnp.bfloat16)
        weight = weight.astype(jnp.bfloat16)
    if out_count <= in_count:
        flattened = weight.reshape(9 * out_count, in_count)
        product = jnp.einsum(
            "kc,xcy->xky", flattened, padded, preferred_element_type=jnp.float32
        )
        product = jnp.pad(product, ((0, 0), (0, 0), (1, 1)))
        summed = jnp.zeros((row_count, out_count, lat_count), jnp.float32)
        for step_lon in range(3):
            for step_lat in range(3):
                tap_index = step_lon * 3 + step_lat
                summed = (
                    summed
                    + product[
                        step_lon : step_lon + row_count,
                        tap_index * out_count : (tap_index + 1) * out_count,
                        step_lat : step_lat + lat_count,
                    ]
                )
        return summed
    lat_padded = jnp.pad(padded, ((0, 0), (0, 0), (1, 1)))
    stacked = jnp.concatenate(
        [
            lat_padded[step_lon : step_lon + row_count, :, step_lat : step_lat + lat_count]
            for step_lon in range(3)
            for step_lat in range(3)
        ],
        axis=1,
    )
    flattened = jnp.transpose(weight, (2, 0, 1, 3)).reshape(out_count, 9 * in_count)
    return jnp.einsum(
        "ok,xky->xoy", flattened, stacked, precision=precision, preferred_element_type=jnp.float32
    )


def split(values):
    high = lax.reduce_precision(values, 8, 7)
    return high.astype(jnp.bfloat16), (values - high).astype(jnp.bfloat16)


def convolve_fine(padded, weight):
    out_count, in_count = weight.shape[2:]
    upper, lower = split(padded)
    weight_upper, weight_lower = split(weight)
    if out_count <= in_count:
        both = jnp.concatenate([upper, lower], axis=1)
        stacked = jnp.concatenate([weight_upper, weight_lower], axis=2)
        stacked = jnp.concatenate([stacked, stacked], axis=3)
        result = convolve(both, stacked)
        return result[:, :out_count] + result[:, out_count:]
    return convolve(padded, weight, lax.Precision.HIGH)


def flipped(weight):
    return jnp.transpose(weight[::-1, ::-1], (0, 1, 3, 2))


def band_matrix(count, wrap):
    row_index = jnp.arange(count)[:, None]
    col_index = jnp.arange(count)[None, :]
    distance = jnp.abs(row_index - col_index)
    if wrap:
        distance = jnp.minimum(distance, count - distance)
    ratio = distance.astype(jnp.float32) / (HALF + 1.0)
    return jnp.where(distance <= HALF, 1.0 - ratio * ratio, 0.0).astype(jnp.bfloat16)


def tile_cols(t):
    return slice(t * LANES, (t + 1) * LANES)


def shifted(values, step):
    if step == 1:
        return values
    width = values.shape[-1]
    column = lax.broadcasted_iota(jnp.int32, values.shape, values.ndim - 1)
    if step == 0:
        return jnp.where(column == 0, 0.0, pltpu.roll(values, 1, values.ndim - 1))
    return jnp.where(column == width - 1, 0.0, pltpu.roll(values, width - 1, values.ndim - 1))


def tap_of(distance):
    ratio = distance / (HALF + 1.0)
    return jnp.where(distance <= HALF, 1.0 - ratio * ratio, 0.0)


def halves(values):
    high = values.astype(jnp.bfloat16)
    return high, (values - high.astype(jnp.float32)).astype(jnp.bfloat16)


def step_kernel(
    count, total_members,
    members_hbm, state_hbm, cot_hbm, win_hbm, wout_hbm, bias_hbm,
    stage_ref,
    mem_ref, own_ref, halo_ref, taps_ref, wraw_ref, bias_ref, slot_ref,
    w_state, w_cot, v_in, w_tail, v_tail,
    slopes_ref, back_ref, part_ref, q_ref, g_ref, whole_ref, lat_ref, lon_ref, rim_ref, banded_ref, contrib_ref,
    out_buf, in_buf, total_ref,
    mem_sem, own_sem, small_sem, halo_send, halo_recv, g_send, g_recv, r_send, r_recv,
):
    me = lax.axis_index("space")
    members, lane_tiles, high_rows, _ = mem_ref.shape
    var_count = wraw_ref.shape[3]
    two = own_ref.shape[2]
    rows = two // var_count
    lats = lane_tiles * LANES
    hidden = slot_ref.shape[2]
    depth = count // 8
    before, after = lax.rem(me + count - 1, count), lax.rem(me + 1, count)

    own_loads = []
    for index, source in enumerate((state_hbm, cot_hbm)):
        for t in range(lane_tiles):
            copy = pltpu.make_async_copy(
                source.reshape(two, lats).at[:, tile_cols(t)],
                own_ref.at[index, t],
                own_sem.at[index, t],
            )
            copy.start()
            own_loads.append(copy)
    small_loads = [
        pltpu.make_async_copy(win_hbm, wraw_ref.at[0], small_sem.at[0]),
        pltpu.make_async_copy(wout_hbm, wraw_ref.at[1], small_sem.at[1]),
        pltpu.make_async_copy(bias_hbm, bias_ref, small_sem.at[2]),
    ]
    for copy in small_loads:
        copy.start()
    mem_loads = []
    flat_members = members_hbm.reshape(members, high_rows, lats)
    for m in range(members):
        for t in range(lane_tiles):
            copy = pltpu.make_async_copy(
                flat_members.at[m, :, tile_cols(t)], mem_ref.at[m, t], mem_sem.at[m, t]
            )
            copy.start()
            mem_loads.append(copy)

    barrier = pltpu.get_barrier_semaphore()
    friends = [before, after] + [flip(me, 1), flip(me, 2), flip(me, 4)]
    friends += [flip_all(me, 8 * j) for j in range(1, depth)]
    for friend in friends:
        pl.semaphore_signal(
            barrier, inc=1, device_id={"space": friend}, device_id_type=pl.DeviceIdType.MESH
        )

    row = lax.broadcasted_iota(jnp.int32, taps_ref.shape[2:], 0)
    blank = jnp.where((row & 7) == 6, 1.0, 0.0)
    for index in range(2):
        for t in range(lane_tiles):
            taps_ref[index, t] = blank
    window = lat_ref.shape[1]
    for index in range(2):
        offset = index * (lats - window)
        y = lax.broadcasted_iota(jnp.int32, (window, window), 0)
        z = lax.broadcasted_iota(jnp.int32, (window, window), 1)
        value = tap_of(jnp.abs(y - z).astype(jnp.float32))
        mine = (z + offset < lats // 2) if index == 0 else (z + offset >= lats // 2)
        lat_ref[index] = jnp.where(mine, value, 0.0).astype(jnp.bfloat16)
    i = lax.broadcasted_iota(jnp.int32, lon_ref.shape, 0)
    j = lax.broadcasted_iota(jnp.int32, lon_ref.shape, 1)
    gap = i - j + var_count * HALF
    value = tap_of(jnp.abs(gap).astype(jnp.float32) * 0.5)
    lon_ref[...] = jnp.where((gap & 1) == 0, value, 0.0).astype(jnp.bfloat16)
    i = lax.broadcasted_iota(jnp.int32, rim_ref.shape, 0)
    j = lax.broadcasted_iota(jnp.int32, rim_ref.shape, 1)
    gap = i - j + rim_ref.shape[1] // 2 - 8
    value = tap_of(jnp.abs(gap).astype(jnp.float32) * 0.5)
    rim_ref[...] = jnp.where((gap & 1) == 0, value, 0.0).astype(jnp.bfloat16)

    for copy in small_loads:
        copy.wait()
    slot_ref[...] = jnp.zeros(slot_ref.shape, jnp.float32)
    for a in range(3):
        for b in range(3):
            place = slice(8 * a + 2 * b, 8 * a + 2 * b + 2)
            slot_ref[0, place, :] = wraw_ref[0, a, b]
            slot_ref[1, place, :] = wraw_ref[0, 2 - a, 2 - b]
            slot_ref[2, place, :] = wraw_ref[1, 2 - a, 2 - b]
            slot_ref[3, place, :] = wraw_ref[1, a, b]
    w_tail[...] = slot_ref[0].T.astype(jnp.bfloat16)
    v_tail[...] = slot_ref[3].astype(jnp.bfloat16)
    slot_ref[0, 14:15, :] = bias_ref[...]
    for target, index in ((w_state, 0), (w_cot, 2)):
        high, low = halves(slot_ref[index].T)
        target[...] = jnp.concatenate([high, high, low], axis=1)
    high, low = halves(slot_ref[1])
    v_in[:32] = jnp.concatenate([high, high], axis=1)
    v_in[32:] = jnp.concatenate([low, low], axis=1)

    for copy in own_loads:
        copy.wait()
    pl.semaphore_wait(barrier, len(friends))
    edges = []
    for side, start, friend in ((1, 0, before), (0, two - 8, after)):
        copy = pltpu.make_async_remote_copy(
            src_ref=own_ref.at[:, :, start : start + 8],
            dst_ref=halo_ref.at[side],
            send_sem=halo_send.at[side],
            recv_sem=halo_recv.at[side],
            device_id={"space": friend},
            device_id_type=pl.DeviceIdType.MESH,
        )
        copy.start()
        edges.append(copy)

    for index in range(2):
        for c in range(var_count):
            values = jnp.concatenate(
                [own_ref[index, t, pl.ds(c, rows, stride=var_count), :] for t in range(lane_tiles)],
                axis=1,
            )
            for b in range(3):
                moved = shifted(values, b)
                for t in range(lane_tiles):
                    taps_ref[index, t, pl.ds(16 + 2 * b + c, rows, stride=8), :] = moved[:, tile_cols(t)]

    def lane_chunks():
        tiles = [(line, t) for line in range(2) for t in range(lane_tiles)]
        return [tiles[k : k + 2] for k in range(0, len(tiles), 2)]

    def tap_block(index, j, t):
        start = 8 * j if isinstance(j, int) else pl.multiple_of(8 * j, 8)
        return taps_ref[index, t, pl.ds(start, 32), :]

    def fine_block(index, j, t):
        high, low = halves(tap_block(index, j, t))
        return jnp.concatenate([high, low, high], axis=0)

    def in_groups(step, first, last, group):
        def several(k, carry):
            for place in range(group):
                step(first + k * group + place)
            return carry

        full = (last - first) // group
        lax.fori_loop(0, full, several, 0)
        for p in range(first + full * group, last):
            step(p)

    def head_pair(p):
        for chunk in lane_chunks():
            lines = [(2 * p + line, t) for line, t in chunk]
            field = jnp.concatenate([fine_block(0, j, t) for j, t in lines], axis=1)
            misfit = jnp.concatenate([fine_block(1, j, t) for j, t in lines], axis=1)
            activity = jnp.tanh(jnp.dot(w_state[...], field, preferred_element_type=jnp.float32))
            slopes = 1.0 - activity * activity
            back = slopes * jnp.dot(w_cot[...], misfit, preferred_element_type=jnp.float32)
            back = jnp.concatenate(halves(back), axis=0)
            for place, (j, t) in enumerate(lines):
                slopes_ref[j, :, tile_cols(t)] = slopes[:, tile_cols(place)]
                back_ref[j, :, tile_cols(t)] = back[:, tile_cols(place)]

    def project_pair(weights, p):
        for chunk in lane_chunks():
            lines = [(2 * p + line, t) for line, t in chunk]
            pieces = jnp.dot(
                weights,
                jnp.concatenate(
                    [back_ref[j, : weights.shape[1], tile_cols(t)] for j, t in lines], axis=1
                ),
                preferred_element_type=jnp.float32,
            )
            if pieces.shape[0] > 32:
                pieces = pieces[:32] + pieces[32:]
            for place, (j, t) in enumerate(lines):
                part_ref[j, :, tile_cols(t)] = pieces[:24, tile_cols(place)]

    pairs = (rows + 2) // 2

    in_groups(head_pair, 1, pairs - 1, HEAD_GROUP)
    in_groups(functools.partial(project_pair, v_in[...]), 1, pairs - 1, HEAD_GROUP)

    for copy in edges:
        copy.wait()
    for side, slot, first in ((0, 0, 4), (1, rows + 2, 0)):
        for index in range(2):
            values = jnp.concatenate(
                [halo_ref[side, index, t] for t in range(lane_tiles)], axis=1
            )
            for b in range(3):
                moved = shifted(values, b)
                for line in range(2):
                    at = 8 * (slot + line) + 2 * b
                    for t in range(lane_tiles):
                        taps_ref[index, t, at : at + 2, :] = moved[
                            first + 2 * line : first + 2 * line + 2, tile_cols(t)
                        ]

    for p in (0, pairs - 1):
        head_pair(p)
    for p in (0, pairs - 1):
        project_pair(v_in[...], p)

    def assembled(c):
        return sum(
            shifted(tile_rows(q_ref, pl.ds(2 * b + c, rows, stride=8)), b) for b in range(3)
        )

    def tile_rows(ref, place):
        return jnp.concatenate([ref[t, place, :] for t in range(lane_tiles)], axis=1)

    def gather_pieces():
        for t in range(lane_tiles):
            cols = tile_cols(t)
            joined = (
                part_ref[0:rows, 0:8, cols]
                + part_ref[1 : rows + 1, 8:16, cols]
                + part_ref[2 : rows + 2, 16:24, cols]
            )
            q_ref[t] = joined.reshape(rows * 8, LANES)

    gather_pieces()
    for c in range(var_count):
        values = jnp.concatenate(
            [own_ref[1, t, pl.ds(c, rows, stride=var_count), :] for t in range(lane_tiles)], axis=1
        )
        values = values + assembled(c)
        for t in range(lane_tiles):
            g_ref[t, pl.ds(c, rows, stride=var_count), :] = values[:, tile_cols(t)]
    whole_ref[me] = tile_rows(g_ref, slice(None)).astype(jnp.bfloat16)

    forks = [j for j in range(depth) if bin(j).count("1") % 2 == 0]
    sends = []

    def pass_on(rel, stride):
        owner = flip_all(me, rel)
        slot = rel ^ stride
        copy = pltpu.make_async_remote_copy(
            src_ref=whole_ref.at[owner],
            dst_ref=whole_ref.at[owner],
            send_sem=g_send.at[len(sends)],
            recv_sem=g_recv.at[slot],
            device_id={"space": flip_all(me, stride)},
            device_id_type=pl.DeviceIdType.MESH,
        )
        copy.start()
        sends.append(copy)

    def await_block(rel):
        owner = flip_all(me, rel)
        pltpu.make_async_remote_copy(
            src_ref=whole_ref.at[owner],
            dst_ref=whole_ref.at[owner],
            send_sem=g_send.at[0],
            recv_sem=g_recv.at[rel],
            device_id={"space": flip(me, 1)},
            device_id_type=pl.DeviceIdType.MESH,
        ).wait_recv()

    pass_on(0, 2)
    pass_on(0, 4)
    for j in range(1, depth):
        pass_on(0, 8 * j)
    pass_on(0, 1)
    for j in range(depth):
        if j:
            await_block(8 * j)
            pass_on(8 * j, 2)
            pass_on(8 * j, 4)
            pass_on(8 * j, 1)
        if j == 0:
            for near in (2, 4):
                await_block(near)
                if (near == 4) == (j in forks):
                    pass_on(near, 6 - near)
                pass_on(near, 1)
    margin = (banded_ref.shape[0] - high_rows) // 2
    group = count // depth
    span = group * two

    def lat_step(d):
        at = pl.multiple_of(d * span, 16)
        fields = [
            whole_ref[pl.ds(d * group, group), :, tile_cols(t)].reshape(span, LANES)
            for t in range(lane_tiles)
        ]
        products = [
            [mem_ref[m, t, pl.ds(at, span), :] * fields[t] for t in range(lane_tiles)]
            for m in range(members)
        ]
        sides = [
            jnp.dot(
                jnp.concatenate(
                    [jnp.concatenate(p[side : side + 2], axis=1) for p in products], axis=0
                ),
                lat_ref[side],
                preferred_element_type=jnp.float32,
            )
            for side in range(2)
        ]
        bands = [
            sides[0][:, :LANES],
            sides[0][:, LANES:] + sides[1][:, :LANES],
            sides[1][:, LANES:],
        ]
        for t, band in enumerate(bands):
            narrow = band.astype(jnp.bfloat16)
            for m in range(members):
                banded_ref[pl.ds(at + margin, span), tile_cols(t * members + m)] = narrow[
                    m * span : (m + 1) * span
                ]

    def near_blocks(j):
        for near in (2, 4):
            rel = 8 * j + near
            await_block(rel)
            if (near == 4) == (j in forks):
                pass_on(rel, 6 - near)
            pass_on(rel, 1)

    for copy in mem_loads:
        copy.wait()
    def finish(j):
        await_block(8 * j + 6)
        pass_on(8 * j + 6, 1)

    def band(j):
        for column in range(1, 8, 2):
            await_block(8 * j + column)
        lat_step(flip_all(me, 8 * j) // 8)

    lead = min(1, depth - 1)
    for j in range(1, depth):
        near_blocks(j)
    for j in range(depth + lead):
        if j < depth:
            finish(j)
        if j >= lead:
            band(j - lead)

    banded_ref[:margin] = banded_ref[high_rows : high_rows + margin]
    banded_ref[high_rows + margin :] = banded_ref[margin : 2 * margin]

    band_rows, band_depth = lon_ref.shape
    inset = margin - (band_depth - band_rows) // 2

    def lon_step(q, carry):
        at = pl.multiple_of(q * band_rows, 16)
        for t in range(lane_tiles):
            total = jnp.zeros((band_rows, LANES), jnp.float32)
            for m in range(0, members, 2):
                start = (t * members + m) * LANES
                spread = jnp.dot(
                    lon_ref[...],
                    banded_ref[pl.ds(at + inset, band_depth), start : start + 2 * LANES],
                    preferred_element_type=jnp.float32,
                )
                for k in range(2):
                    total += (
                        mem_ref[m + k, t, pl.ds(at, band_rows), :].astype(jnp.float32)
                        * spread[:, tile_cols(k)]
                    )
            contrib_ref[pl.ds(at + 8, band_rows), tile_cols(t)] = total
        return carry

    def lon_plane(p):
        per = span // band_rows
        lax.fori_loop(p * per, (p + 1) * per, lon_step, 0)

    for p in range(depth):
        at = p * span
        ahead = (at - 8) % high_rows
        for t in range(lane_tiles):
            total = jnp.zeros((16, LANES), jnp.float32)
            for m in range(0, members, 2):
                start = (t * members + m) * LANES
                spread = jnp.dot(
                    rim_ref[...],
                    banded_ref[at : at + 2 * margin, start : start + 2 * LANES],
                    preferred_element_type=jnp.float32,
                )
                for k in range(2):
                    near = jnp.concatenate(
                        [
                            mem_ref[m + k, t, ahead : ahead + 8, :].astype(jnp.float32),
                            mem_ref[m + k, t, at : at + 8, :].astype(jnp.float32),
                        ],
                        axis=0,
                    )
                    total += near * spread[:, tile_cols(k)]
            contrib_ref[at : at + 16, tile_cols(t)] = total
            if p == 0:
                contrib_ref[high_rows + 8 :, tile_cols(t)] = total[8:]

    for copy in sends:
        copy.wait_send()

    def part_of(rel):
        at = pl.multiple_of(flip_all(me, rel) * two, 16)
        body = contrib_ref[pl.ds(at + 8, two), :]
        ahead = contrib_ref[pl.ds(at, 8), :]
        behind = contrib_ref[pl.ds(at + 8 + two, 8), :]
        row = lax.broadcasted_iota(jnp.int32, (8, lats), 0)
        return body, jnp.where(row < 4, behind, ahead)

    reduce_sends = []

    def ship(value, slot, stride):
        out_buf[slot, :two] = value[0].astype(jnp.bfloat16)
        out_buf[slot, two:] = value[1].astype(jnp.bfloat16)
        copy = pltpu.make_async_remote_copy(
            src_ref=out_buf.at[slot],
            dst_ref=in_buf.at[slot],
            send_sem=r_send.at[slot],
            recv_sem=r_recv.at[slot],
            device_id={"space": flip_all(me, stride)},
            device_id_type=pl.DeviceIdType.MESH,
        )
        copy.start()
        reduce_sends.append(copy)
        return copy

    flying = {}

    def arrived(value, slot):
        flying[slot].wait_recv()
        return (
            value[0] + in_buf[slot, :two].astype(jnp.float32),
            value[1] + in_buf[slot, two:].astype(jnp.float32),
        )

    column_of = {6: 0, 2: 1, 4: 2, 0: 3}
    far = list(range(depth))[::-1]
    base = 4 * depth
    last = base + 3 * depth

    def to_partner(j):
        lon_plane(flip_all(me, 8 * j) // 8)
        for column in (6, 2, 4, 0):
            slot = column_of[column] * depth + j
            flying[slot] = ship(part_of(8 * j + column + 1), slot, 1)

    def chip_part(column, j):
        return arrived(part_of(8 * j + column), column_of[column] * depth + j)

    def to_sides(j):
        first = 2 if j in forks else 4
        flying[base + j] = ship(chip_part(6, j), base + j, first)
        slot = base + first // 2 * depth + j
        flying[slot] = ship(chip_part(first, j), slot, first)

    def relayed(j):
        second = 4 if j in forks else 2
        slot = base + second // 2 * depth + j
        flying[slot] = ship(arrived(chip_part(second, j), base + j), slot, second)

    def column_sum(j):
        value = chip_part(0, j)
        for column in (2, 4):
            value = arrived(value, base + column // 2 * depth + j)
        return value

    def along(j):
        if j:
            flying[last + j] = ship(column_sum(j), last + j, 8 * j)

    for step in range(depth + 3):
        for lag, action in enumerate((to_partner, to_sides, relayed, along)):
            if 0 <= step - lag < depth:
                action(far[step - lag])
    value = column_sum(0)
    for j in range(1, depth):
        value = arrived(value, last + j)
    body = value[0] / (total_members - 1.0)
    rim = value[1] / (total_members - 1.0)
    for t in range(lane_tiles):
        total_ref[t, 0:8, :] = rim[:, tile_cols(t)]
        total_ref[t, 8 : 8 + two, :] = body[:, tile_cols(t)]
        total_ref[t, 8 + two :, :] = rim[:, tile_cols(t)]
        stage_ref[0, t] = body[:, tile_cols(t)]
    wide = rows + 4
    for c in range(var_count):
        values = tile_rows(total_ref, pl.ds(4 + c, wide, stride=var_count))
        for b in range(3):
            moved = shifted(values, b)
            for t in range(lane_tiles):
                taps_ref[0, t, pl.ds(2 * b + c, wide, stride=8), :] = moved[:, tile_cols(t)]

    def tail_pair(p):
        for chunk in lane_chunks():
            lines = [(2 * p + line, t) for line, t in chunk]
            field = jnp.concatenate([tap_block(0, j, t) for j, t in lines], axis=1)
            tangent = jnp.dot(
                w_tail[...], field.astype(jnp.bfloat16), preferred_element_type=jnp.float32
            )
            slopes = jnp.concatenate([slopes_ref[j, :, tile_cols(t)] for j, t in lines], axis=1)
            back = (slopes * tangent).astype(jnp.bfloat16)
            for place, (j, t) in enumerate(lines):
                back_ref[j, :hidden, tile_cols(t)] = back[:, tile_cols(place)]

    in_groups(tail_pair, 0, pairs, TAIL_GROUP)
    in_groups(functools.partial(project_pair, v_tail[...]), 0, pairs, TAIL_GROUP)
    gather_pieces()
    for c in range(var_count):
        values = tile_rows(total_ref, pl.ds(8 + c, rows, stride=var_count)) + assembled(c)
        for t in range(lane_tiles):
            stage_ref[1, t, pl.ds(c, rows, stride=var_count), :] = values[:, tile_cols(t)]
    for copy in reduce_sends:
        copy.wait_send()


def emit_kernel(tiled_ref, incr_hbm, resp_hbm, out_sem):
    _, tiles, two, _ = tiled_ref.shape
    stores = []
    for index, target in enumerate((incr_hbm, resp_hbm)):
        for t in range(tiles):
            copy = pltpu.make_async_copy(
                tiled_ref.at[index, t],
                target.reshape(two, tiles * LANES).at[:, tile_cols(t)],
                out_sem.at[index, t],
            )
            copy.start()
            stores.append(copy)
    for copy in stores:
        copy.wait()


def whole_step(members, state, cotangent, conv_in, conv_out, bias):
    count = lax.axis_size("space")
    mine, lons, var_count, lats = members.shape
    rows = state.shape[0]
    hidden = bias.shape[0]
    two = rows * var_count
    tiles = lats // LANES
    depth = count // 8
    any_space = pl.BlockSpec(memory_space=pl.ANY)
    vmem = pltpu.VMEM
    dma = pltpu.SemaphoreType.DMA
    margin = HALF * var_count
    window = lats - LANES
    slots = 8 * depth
    tiled = pl.pallas_call(
        functools.partial(step_kernel, count, mine * count),
        out_shape=jax.ShapeDtypeStruct((2, tiles, two, LANES), jnp.float32),
        in_specs=[any_space] * 6,
        out_specs=pl.BlockSpec(memory_space=vmem),
        scratch_shapes=[
            vmem((mine, tiles, lons * var_count, LANES), jnp.bfloat16),
            vmem((2, tiles, two, LANES), jnp.float32),
            vmem((2, 2, tiles, 8, LANES), jnp.float32),
            vmem((2, tiles, (rows + 5) * 8, LANES), jnp.float32),
            vmem((2, 3, 3, var_count, hidden), jnp.float32),
            vmem((1, hidden), jnp.float32),
            vmem((4, 32, hidden), jnp.float32),
            vmem((hidden, 96), jnp.bfloat16),
            vmem((hidden, 96), jnp.bfloat16),
            vmem((64, 2 * hidden), jnp.bfloat16),
            vmem((hidden, 32), jnp.bfloat16),
            vmem((32, hidden), jnp.bfloat16),
            vmem((rows + 2, hidden, lats), jnp.float32),
            vmem((rows + 2, 2 * hidden, lats), jnp.bfloat16),
            vmem((rows + 2, 24, lats), jnp.float32),
            vmem((tiles, rows * 8, LANES), jnp.float32),
            vmem((tiles, two, LANES), jnp.float32),
            vmem((count, two, lats), jnp.bfloat16),
            vmem((2, window, window), jnp.bfloat16),
            vmem((4 * two, 4 * two + 2 * margin), jnp.bfloat16),
            vmem((16, 2 * (margin + 16)), jnp.bfloat16),
            vmem((lons * var_count + 2 * (margin + 16), mine * lats), jnp.bfloat16),
            vmem((lons * var_count + 16, lats), jnp.float32),
            vmem((slots, two + 8, lats), jnp.bfloat16),
            vmem((slots, two + 8, lats), jnp.bfloat16),
            vmem((tiles, two + 16, LANES), jnp.float32),
            dma((mine, tiles)),
            dma((2, tiles)),
            dma((3,)),
            dma((2,)),
            dma((2,)),
            dma((count,)),
            dma((count,)),
            dma((slots,)),
            dma((slots,)),
        ],
        compiler_params=pltpu.CompilerParams(collective_id=2, has_side_effects=True),
        name="whole_step",
    )(
        members,
        state,
        cotangent,
        jnp.transpose(conv_in, (0, 1, 3, 2)),
        conv_out,
        bias.reshape(1, hidden),
    )
    return pl.pallas_call(
        emit_kernel,
        out_shape=(jax.ShapeDtypeStruct(state.shape, jnp.float32),) * 2,
        in_specs=[pl.BlockSpec(memory_space=vmem)],
        out_specs=(any_space,) * 2,
        scratch_shapes=[dma((2, tiles))],
        name="emit",
    )(tiled)


def fits(members, state, bias):
    count = lax.axis_size("space")
    mine, lons, var_count, lats = members.shape
    rows = state.shape[0]
    return (
        lax.axis_size("mem") == 1
        and count >= 8
        and count & (count - 1) == 0
        and var_count == 2
        and lats == 3 * LANES
        and rows % 8 == 0
        and rows >= 2 * 8
        and mine % 2 == 0
        and lons == count * rows
        and bias.shape[0] == LANES
    )


def per_device(members, state, cotangent, conv_in, conv_out, bias):
    row_count, var_count, lat_count = state.shape
    if fits(members, state, bias):
        return whole_step(members, state, cotangent, conv_in, conv_out, bias)
    count = lax.axis_size("space")
    direct = count >= 8 and count & (count - 1) == 0
    rim_width = 2
    joined = jnp.concatenate([state, cotangent], axis=1)
    padded = padded_2(joined, "space", rim_width)
    state_pad = padded[:, :var_count]
    cot_pad = padded[:, var_count:]
    activity = jnp.tanh(convolve_fine(state_pad, conv_in) + bias[None, :, None])
    slopes = 1.0 - activity * activity
    backward = slopes * convolve_fine(cot_pad, flipped(conv_out))
    gradient = cotangent + convolve_fine(backward, flipped(conv_in))
    gradient = gradient.astype(jnp.bfloat16)
    width = var_count * lat_count
    gradient = gradient.reshape(row_count, width)
    if direct:
        whole = gather(gradient).reshape(count * row_count, width)
    else:
        whole = lax.all_gather(gradient, "space", axis=0, tiled=True)
    merged = members.reshape(members.shape[0], members.shape[1], width)
    lat_loc = band_matrix(lat_count, False)
    lon_loc = band_matrix(merged.shape[1], True)
    contrib = covariance(merged, whole, lat_loc, lon_loc)
    member_count = members.shape[0] * lax.axis_size("space") * lax.axis_size("mem")
    if direct:
        own, left, right = scatter(
            contrib.reshape(count, row_count, width), rim_width
        )
        total = jnp.concatenate([left, own, right], axis=0)
        total = total.reshape(row_count + 2 * rim_width, var_count, lat_count)
        if lax.axis_size("mem") > 1:
            total = lax.psum(total, "mem")
        incr_pad = total / (member_count - 1.0)
        increment = incr_pad[rim_width : rim_width + row_count]
    else:
        member_sum = lax.psum(contrib, "mem")
        block_sum = lax.psum_scatter(member_sum, "space", scatter_dimension=0, tiled=True)
        increment = block_sum.reshape(state.shape) / (member_count - 1.0)
        incr_pad = padded_2(increment, "space", rim_width)
    tangent_hidden = slopes * convolve(incr_pad, conv_in)
    response = increment + convolve(tangent_hidden, conv_out)
    return (increment, response)


def solution(mesh):
    in_specs = (
        P(("space", "mem"), None, None, None),
        P("space", None, None),
        P("space", None, None),
        P(),
        P(),
        P(),
    )
    out_specs = (P("space", None, None), P("space", None, None))
    return jax.shard_map(
        per_device, mesh=mesh, in_specs=in_specs, out_specs=out_specs, check_vma=False
    )
```

```python
import functools

import jax
import jax.numpy as jnp
from jax import lax
from jax.experimental import pallas as pl
from jax.experimental.pallas import tpu as pltpu
from jax.sharding import PartitionSpec as P

HALF = 16
LANES = 128
HEAD_GROUP = 11
TAIL_GROUP = 13


def flip(index, stride):
    return index + stride * (1 - 2 * lax.rem(index // stride, 2))


def flip_all(index, mask):
    stride = 1
    while stride <= mask:
        if mask & stride:
            index = flip(index, stride)
        stride *= 2
    return index


def stages_of(count):
    held = [0]
    steps = []
    stride = count // 2
    while stride >= 8:
        steps.append([(stride, list(held))])
        held = held + [m ^ stride for m in held]
        stride //= 2
    half = max(1, len(held) // 2)
    first, second = held[:half], held[half:]
    steps.append([(2, first), (4, second)])
    first = first + [m ^ 2 for m in first]
    second = second + [m ^ 4 for m in second]
    steps.append([(4, first), (2, second)])
    return steps


def greet(me, count, extra=()):
    barrier = pltpu.get_barrier_semaphore()
    friends = list(extra)
    stride = 1
    while stride < count:
        friends.append(flip(me, stride))
        stride *= 2
    for friend in friends:
        pl.semaphore_signal(
            barrier, inc=1, device_id={"space": friend}, device_id_type=pl.DeviceIdType.MESH
        )
    pl.semaphore_wait(barrier, len(friends))


def gather_kernel(count, block_ref, whole_ref, send_sem, recv_sem):
    me = lax.axis_index("space")
    greet(me, count)

    def remote(mask, stride):
        owner = flip_all(me, mask)
        source = block_ref if mask == 0 else whole_ref.at[owner]
        slot = mask ^ stride
        return pltpu.make_async_remote_copy(
            src_ref=source,
            dst_ref=whole_ref.at[owner],
            send_sem=send_sem.at[slot],
            recv_sem=recv_sem.at[slot],
            device_id={"space": flip(me, stride)},
            device_id_type=pl.DeviceIdType.MESH,
        )

    started = []
    pair = []
    for step in stages_of(count):
        now = []
        for position in range(max(len(masks) for stride, masks in step)):
            for stride, masks in step:
                if position < len(masks):
                    copy = remote(masks[position], stride)
                    copy.start()
                    now.append((copy, masks[position] ^ stride))
        if not pair:
            copy = remote(0, 1)
            copy.start()
            pair.append(copy)
            whole_ref[me] = block_ref[...]
        for copy, mask in now:
            copy.wait_recv()
            other = remote(mask, 1)
            other.start()
            pair.append(other)
            started.append(copy)
    for copy in started:
        copy.wait_send()
    for copy in pair:
        copy.wait()


def gather(block):
    count = lax.axis_size("space")
    return pl.pallas_call(
        functools.partial(gather_kernel, count),
        out_shape=jax.ShapeDtypeStruct((count,) + block.shape, block.dtype),
        in_specs=[pl.BlockSpec(memory_space=pltpu.VMEM)],
        out_specs=pl.BlockSpec(memory_space=pltpu.VMEM),
        scratch_shapes=[
            pltpu.SemaphoreType.DMA((count,)),
            pltpu.SemaphoreType.DMA((count,)),
        ],
        compiler_params=pltpu.CompilerParams(collective_id=0, has_side_effects=True),
        name="gather",
    )(block)


def scatter_kernel(
    count, rim, part_ref, sum_ref, left_ref, right_ref,
    out_buf, in_buf, edge_buf, send_sem, recv_sem, edge_send, edge_recv,
):
    me = lax.axis_index("space")
    before, after = lax.rem(me + count - 1, count), lax.rem(me + 1, count)
    greet(me, count, (before, after))
    arrived = {mask: [] for mask in range(count)}

    def value(mask):
        total = part_ref[flip_all(me, mask)]
        for slot in arrived[mask]:
            total = total + in_buf[slot].astype(jnp.float32)
        return total

    sent = []
    for step in [[(1, list(range(0, count, 2)))]] + stages_of(count)[::-1]:
        now = []
        for position in range(max(len(masks) for stride, masks in step)):
            for stride, masks in step:
                if position < len(masks):
                    slot = masks[position] ^ stride
                    out_buf[slot] = value(slot).astype(out_buf.dtype)
                    copy = pltpu.make_async_remote_copy(
                        src_ref=out_buf.at[slot],
                        dst_ref=in_buf.at[slot],
                        send_sem=send_sem.at[slot],
                        recv_sem=recv_sem.at[slot],
                        device_id={"space": flip(me, stride)},
                        device_id_type=pl.DeviceIdType.MESH,
                    )
                    copy.start()
                    now.append((copy, masks[position], slot))
        for copy, mask, slot in now:
            copy.wait_recv()
            arrived[mask].append(slot)
            sent.append(copy)
    total = value(0)
    sum_ref[...] = total
    edge_buf[0] = total[:rim]
    edge_buf[1] = total[total.shape[0] - rim :]
    edges = [
        pltpu.make_async_remote_copy(
            src_ref=edge_buf.at[side],
            dst_ref=target,
            send_sem=edge_send.at[side],
            recv_sem=edge_recv.at[side],
            device_id={"space": friend},
            device_id_type=pl.DeviceIdType.MESH,
        )
        for side, target, friend in ((0, right_ref, before), (1, left_ref, after))
    ]
    for copy in edges:
        copy.start()
    for copy in sent:
        copy.wait_send()
    for copy in edges:
        copy.wait()


def scatter(parts, rim):
    count, rows, lat_count = parts.shape
    return pl.pallas_call(
        functools.partial(scatter_kernel, count, rim),
        out_shape=(
            jax.ShapeDtypeStruct((rows, lat_count), jnp.float32),
            jax.ShapeDtypeStruct((rim, lat_count), jnp.float32),
            jax.ShapeDtypeStruct((rim, lat_count), jnp.float32),
        ),
        in_specs=[pl.BlockSpec(memory_space=pltpu.VMEM)],
        out_specs=(pl.BlockSpec(memory_space=pltpu.VMEM),) * 3,
        scratch_shapes=[
            pltpu.VMEM((count, rows, lat_count), jnp.bfloat16),
            pltpu.VMEM((count, rows, lat_count), jnp.bfloat16),
            pltpu.VMEM((2, rim, lat_count), jnp.float32),
            pltpu.SemaphoreType.DMA((count,)),
            pltpu.SemaphoreType.DMA((count,)),
            pltpu.SemaphoreType.DMA((2,)),
            pltpu.SemaphoreType.DMA((2,)),
        ],
        compiler_params=pltpu.CompilerParams(collective_id=1, has_side_effects=True),
        name="scatter",
    )(parts)


def covariance_kernel(members_ref, whole_ref, lat_ref, lon_ref, sum_ref, banded_ref):
    lat_count = lat_ref.shape[0]

    @pl.when(pl.program_id(0) == 0)
    def _():
        sum_ref[...] = jnp.zeros_like(sum_ref)

    for start in range(0, whole_ref.shape[1], lat_count):
        columns = slice(start, start + lat_count)
        product = members_ref[0, :, columns].astype(jnp.float32) * whole_ref[:, columns].astype(
            jnp.float32
        )
        banded_ref[:, columns] = jnp.dot(
            product.astype(jnp.bfloat16), lat_ref[...], preferred_element_type=jnp.float32
        ).astype(jnp.bfloat16)
    for start in range(0, whole_ref.shape[1], lat_count):
        columns = slice(start, start + lat_count)
        spread = jnp.dot(
            lon_ref[...], banded_ref[:, columns], preferred_element_type=jnp.float32
        )
        sum_ref[:, columns] += members_ref[0, :, columns].astype(jnp.float32) * spread


def covariance(members, whole, lat_loc, lon_loc):
    count, lon_count, width = members.shape
    return pl.pallas_call(
        covariance_kernel,
        grid=(count,),
        out_shape=jax.ShapeDtypeStruct((lon_count, width), jnp.float32),
        in_specs=[
            pl.BlockSpec((1, lon_count, width), lambda m: (m, 0, 0)),
            pl.BlockSpec(whole.shape, lambda m: (0, 0)),
            pl.BlockSpec(lat_loc.shape, lambda m: (0, 0)),
            pl.BlockSpec(lon_loc.shape, lambda m: (0, 0)),
        ],
        out_specs=pl.BlockSpec((lon_count, width), lambda m: (0, 0)),
        scratch_shapes=[pltpu.VMEM((lon_count, width), jnp.bfloat16)],
        name="covariance",
    )(members, whole, lat_loc, lon_loc)


def padded_2(cells, axis, width):
    count = lax.axis_size(axis)
    head = cells[:width]
    tail = cells[cells.shape[0] - width :]
    return jnp.concatenate(
        [
            lax.ppermute(tail, axis, [(i, (i + 1) % count) for i in range(count)]),
            cells,
            lax.ppermute(head, axis, [((i + 1) % count, i) for i in range(count)]),
        ],
        axis=0,
    )


def convolve(padded, weight, precision=None):
    row_count = padded.shape[0] - 2
    lat_count = padded.shape[2]
    out_count = weight.shape[2]
    in_count = weight.shape[3]
    if precision is None:
        padded = padded.astype(jnp.bfloat16)
        weight = weight.astype(jnp.bfloat16)
    if out_count <= in_count:
        flattened = weight.reshape(9 * out_count, in_count)
        product = jnp.einsum(
            "kc,xcy->xky", flattened, padded, preferred_element_type=jnp.float32
        )
        product = jnp.pad(product, ((0, 0), (0, 0), (1, 1)))
        summed = jnp.zeros((row_count, out_count, lat_count), jnp.float32)
        for step_lon in range(3):
            for step_lat in range(3):
                tap_index = step_lon * 3 + step_lat
                summed = (
                    summed
                    + product[
                        step_lon : step_lon + row_count,
                        tap_index * out_count : (tap_index + 1) * out_count,
                        step_lat : step_lat + lat_count,
                    ]
                )
        return summed
    lat_padded = jnp.pad(padded, ((0, 0), (0, 0), (1, 1)))
    stacked = jnp.concatenate(
        [
            lat_padded[step_lon : step_lon + row_count, :, step_lat : step_lat + lat_count]
            for step_lon in range(3)
            for step_lat in range(3)
        ],
        axis=1,
    )
    flattened = jnp.transpose(weight, (2, 0, 1, 3)).reshape(out_count, 9 * in_count)
    return jnp.einsum(
        "ok,xky->xoy", flattened, stacked, precision=precision, preferred_element_type=jnp.float32
    )


def split(values):
    high = lax.reduce_precision(values, 8, 7)
    return high.astype(jnp.bfloat16), (values - high).astype(jnp.bfloat16)


def convolve_fine(padded, weight):
    out_count, in_count = weight.shape[2:]
    upper, lower = split(padded)
    weight_upper, weight_lower = split(weight)
    if out_count <= in_count:
        both = jnp.concatenate([upper, lower], axis=1)
        stacked = jnp.concatenate([weight_upper, weight_lower], axis=2)
        stacked = jnp.concatenate([stacked, stacked], axis=3)
        result = convolve(both, stacked)
        return result[:, :out_count] + result[:, out_count:]
    return convolve(padded, weight, lax.Precision.HIGH)


def flipped(weight):
    return jnp.transpose(weight[::-1, ::-1], (0, 1, 3, 2))


def band_matrix(count, wrap):
    row_index = jnp.arange(count)[:, None]
    col_index = jnp.arange(count)[None, :]
    distance = jnp.abs(row_index - col_index)
    if wrap:
        distance = jnp.minimum(distance, count - distance)
    ratio = distance.astype(jnp.float32) / (HALF + 1.0)
    return jnp.where(distance <= HALF, 1.0 - ratio * ratio, 0.0).astype(jnp.bfloat16)


def tile_cols(t):
    return slice(t * LANES, (t + 1) * LANES)


def shifted(values, step):
    if step == 1:
        return values
    width = values.shape[-1]
    column = lax.broadcasted_iota(jnp.int32, values.shape, values.ndim - 1)
    if step == 0:
        return jnp.where(column == 0, 0.0, pltpu.roll(values, 1, values.ndim - 1))
    return jnp.where(column == width - 1, 0.0, pltpu.roll(values, width - 1, values.ndim - 1))


def tap_of(distance):
    ratio = distance / (HALF + 1.0)
    return jnp.where(distance <= HALF, 1.0 - ratio * ratio, 0.0)


def halves(values):
    high = values.astype(jnp.bfloat16)
    return high, (values - high.astype(jnp.float32)).astype(jnp.bfloat16)


def step_kernel(
    count, total_members,
    members_hbm, state_hbm, cot_hbm, win_hbm, wout_hbm, bias_hbm,
    stage_ref,
    mem_ref, own_ref, halo_ref, taps_ref, wraw_ref, bias_ref, slot_ref,
    w_state, w_cot, v_in, w_tail, v_tail,
    slopes_ref, back_ref, part_ref, q_ref, g_ref, whole_ref, lat_ref, lon_ref, rim_ref, banded_ref, contrib_ref,
    out_buf, in_buf, total_ref,
    mem_sem, own_sem, small_sem, halo_send, halo_recv, g_send, g_recv, r_send, r_recv,
):
    me = lax.axis_index("space")
    members, lane_tiles, high_rows, _ = mem_ref.shape
    var_count = wraw_ref.shape[3]
    two = own_ref.shape[2]
    rows = two // var_count
    lats = lane_tiles * LANES
    hidden = slot_ref.shape[2]
    depth = count // 8
    before, after = lax.rem(me + count - 1, count), lax.rem(me + 1, count)

    own_loads = []
    for index, source in enumerate((state_hbm, cot_hbm)):
        for t in range(lane_tiles):
            copy = pltpu.make_async_copy(
                source.reshape(two, lats).at[:, tile_cols(t)],
                own_ref.at[index, t],
                own_sem.at[index, t],
            )
            copy.start()
            own_loads.append(copy)
    small_loads = [
        pltpu.make_async_copy(win_hbm, wraw_ref.at[0], small_sem.at[0]),
        pltpu.make_async_copy(wout_hbm, wraw_ref.at[1], small_sem.at[1]),
        pltpu.make_async_copy(bias_hbm, bias_ref, small_sem.at[2]),
    ]
    for copy in small_loads:
        copy.start()
    mem_loads = []
    flat_members = members_hbm.reshape(members, high_rows, lats)
    for m in range(members):
        for t in range(lane_tiles):
            copy = pltpu.make_async_copy(
                flat_members.at[m, :, tile_cols(t)], mem_ref.at[m, t], mem_sem.at[m, t]
            )
            copy.start()
            mem_loads.append(copy)

    barrier = pltpu.get_barrier_semaphore()
    friends = [before, after, flip(me, 1), flip(me, 2), flip(me, 4), flip_all(me, 6)]
    friends += [flip_all(me, 8 * j) for j in range(1, depth)]
    for friend in friends:
        pl.semaphore_signal(
            barrier, inc=1, device_id={"space": friend}, device_id_type=pl.DeviceIdType.MESH
        )

    row = lax.broadcasted_iota(jnp.int32, taps_ref.shape[2:], 0)
    blank = jnp.where((row & 7) == 6, 1.0, 0.0)
    for index in range(2):
        for t in range(lane_tiles):
            taps_ref[index, t] = blank
    window = lat_ref.shape[1]
    for index in range(2):
        offset = index * (lats - window)
        y = lax.broadcasted_iota(jnp.int32, (window, window), 0)
        z = lax.broadcasted_iota(jnp.int32, (window, window), 1)
        value = tap_of(jnp.abs(y - z).astype(jnp.float32))
        mine = (z + offset < lats // 2) if index == 0 else (z + offset >= lats // 2)
        lat_ref[index] = jnp.where(mine, value, 0.0).astype(jnp.bfloat16)
    i = lax.broadcasted_iota(jnp.int32, lon_ref.shape, 0)
    j = lax.broadcasted_iota(jnp.int32, lon_ref.shape, 1)
    gap = i - j + var_count * HALF
    value = tap_of(jnp.abs(gap).astype(jnp.float32) * 0.5)
    lon_ref[...] = jnp.where((gap & 1) == 0, value, 0.0).astype(jnp.bfloat16)
    i = lax.broadcasted_iota(jnp.int32, rim_ref.shape, 0)
    j = lax.broadcasted_iota(jnp.int32, rim_ref.shape, 1)
    gap = i - j + rim_ref.shape[1] // 2 - 8
    value = tap_of(jnp.abs(gap).astype(jnp.float32) * 0.5)
    rim_ref[...] = jnp.where((gap & 1) == 0, value, 0.0).astype(jnp.bfloat16)

    for copy in small_loads:
        copy.wait()
    slot_ref[...] = jnp.zeros(slot_ref.shape, jnp.float32)
    for a in range(3):
        for b in range(3):
            place = slice(8 * a + 2 * b, 8 * a + 2 * b + 2)
            slot_ref[0, place, :] = wraw_ref[0, a, b]
            slot_ref[1, place, :] = wraw_ref[0, 2 - a, 2 - b]
            slot_ref[2, place, :] = wraw_ref[1, 2 - a, 2 - b]
            slot_ref[3, place, :] = wraw_ref[1, a, b]
    w_tail[...] = slot_ref[0].T.astype(jnp.bfloat16)
    v_tail[...] = slot_ref[3].astype(jnp.bfloat16)
    slot_ref[0, 14:15, :] = bias_ref[...]
    for target, index in ((w_state, 0), (w_cot, 2)):
        high, low = halves(slot_ref[index].T)
        target[...] = jnp.concatenate([high, high, low], axis=1)
    high, low = halves(slot_ref[1])
    v_in[:32] = jnp.concatenate([high, high], axis=1)
    v_in[32:] = jnp.concatenate([low, low], axis=1)

    for copy in own_loads:
        copy.wait()
    pl.semaphore_wait(barrier, len(friends))
    edges = []
    for side, start, friend in ((1, 0, before), (0, two - 8, after)):
        copy = pltpu.make_async_remote_copy(
            src_ref=own_ref.at[:, :, start : start + 8],
            dst_ref=halo_ref.at[side],
            send_sem=halo_send.at[side],
            recv_sem=halo_recv.at[side],
            device_id={"space": friend},
            device_id_type=pl.DeviceIdType.MESH,
        )
        copy.start()
        edges.append(copy)

    for index in range(2):
        for c in range(var_count):
            values = jnp.concatenate(
                [own_ref[index, t, pl.ds(c, rows, stride=var_count), :] for t in range(lane_tiles)],
                axis=1,
            )
            for b in range(3):
                moved = shifted(values, b)
                for t in range(lane_tiles):
                    taps_ref[index, t, pl.ds(16 + 2 * b + c, rows, stride=8), :] = moved[:, tile_cols(t)]

    def lane_chunks():
        tiles = [(line, t) for line in range(2) for t in range(lane_tiles)]
        return [tiles[k : k + 2] for k in range(0, len(tiles), 2)]

    def tap_block(index, j, t):
        start = 8 * j if isinstance(j, int) else pl.multiple_of(8 * j, 8)
        return taps_ref[index, t, pl.ds(start, 32), :]

    def fine_block(index, j, t):
        high, low = halves(tap_block(index, j, t))
        return jnp.concatenate([high, low, high], axis=0)

    def in_groups(step, first, last, group):
        def several(k, carry):
            for place in range(group):
                step(first + k * group + place)
            return carry

        full = (last - first) // group
        lax.fori_loop(0, full, several, 0)
        for p in range(first + full * group, last):
            step(p)

    def head_pair(p):
        for chunk in lane_chunks():
            lines = [(2 * p + line, t) for line, t in chunk]
            field = jnp.concatenate([fine_block(0, j, t) for j, t in lines], axis=1)
            misfit = jnp.concatenate([fine_block(1, j, t) for j, t in lines], axis=1)
            activity = jnp.tanh(jnp.dot(w_state[...], field, preferred_element_type=jnp.float32))
            slopes = 1.0 - activity * activity
            back = slopes * jnp.dot(w_cot[...], misfit, preferred_element_type=jnp.float32)
            back = jnp.concatenate(halves(back), axis=0)
            for place, (j, t) in enumerate(lines):
                slopes_ref[j, :, tile_cols(t)] = slopes[:, tile_cols(place)]
                back_ref[j, :, tile_cols(t)] = back[:, tile_cols(place)]

    def project_pair(weights, p):
        for chunk in lane_chunks():
            lines = [(2 * p + line, t) for line, t in chunk]
            pieces = jnp.dot(
                weights,
                jnp.concatenate(
                    [back_ref[j, : weights.shape[1], tile_cols(t)] for j, t in lines], axis=1
                ),
                preferred_element_type=jnp.float32,
            )
            if pieces.shape[0] > 32:
                pieces = pieces[:32] + pieces[32:]
            for place, (j, t) in enumerate(lines):
                part_ref[j, :, tile_cols(t)] = pieces[:24, tile_cols(place)]

    pairs = (rows + 2) // 2

    in_groups(head_pair, 1, pairs - 1, HEAD_GROUP)
    in_groups(functools.partial(project_pair, v_in[...]), 1, pairs - 1, HEAD_GROUP)

    for copy in edges:
        copy.wait()
    for side, slot, first in ((0, 0, 4), (1, rows + 2, 0)):
        for index in range(2):
            values = jnp.concatenate(
                [halo_ref[side, index, t] for t in range(lane_tiles)], axis=1
            )
            for b in range(3):
                moved = shifted(values, b)
                for line in range(2):
                    at = 8 * (slot + line) + 2 * b
                    for t in range(lane_tiles):
                        taps_ref[index, t, at : at + 2, :] = moved[
                            first + 2 * line : first + 2 * line + 2, tile_cols(t)
                        ]

    for p in (0, pairs - 1):
        head_pair(p)
    for p in (0, pairs - 1):
        project_pair(v_in[...], p)

    def assembled(c):
        return sum(
            shifted(tile_rows(q_ref, pl.ds(2 * b + c, rows, stride=8)), b) for b in range(3)
        )

    def tile_rows(ref, place):
        return jnp.concatenate([ref[t, place, :] for t in range(lane_tiles)], axis=1)

    def gather_pieces():
        for t in range(lane_tiles):
            cols = tile_cols(t)
            joined = (
                part_ref[0:rows, 0:8, cols]
                + part_ref[1 : rows + 1, 8:16, cols]
                + part_ref[2 : rows + 2, 16:24, cols]
            )
            q_ref[t] = joined.reshape(rows * 8, LANES)

    gather_pieces()
    for c in range(var_count):
        values = jnp.concatenate(
            [own_ref[1, t, pl.ds(c, rows, stride=var_count), :] for t in range(lane_tiles)], axis=1
        )
        values = values + assembled(c)
        for t in range(lane_tiles):
            g_ref[t, pl.ds(c, rows, stride=var_count), :] = values[:, tile_cols(t)]
    whole_ref[me] = tile_rows(g_ref, slice(None)).astype(jnp.bfloat16)

    forks = [j for j in range(depth) if bin(j).count("1") % 2 == 0]
    sends = []

    def pass_on(rel, stride):
        owner = flip_all(me, rel)
        slot = rel ^ stride
        copy = pltpu.make_async_remote_copy(
            src_ref=whole_ref.at[owner],
            dst_ref=whole_ref.at[owner],
            send_sem=g_send.at[len(sends)],
            recv_sem=g_recv.at[slot],
            device_id={"space": flip_all(me, stride)},
            device_id_type=pl.DeviceIdType.MESH,
        )
        copy.start()
        sends.append(copy)

    def await_block(rel):
        owner = flip_all(me, rel)
        pltpu.make_async_remote_copy(
            src_ref=whole_ref.at[owner],
            dst_ref=whole_ref.at[owner],
            send_sem=g_send.at[0],
            recv_sem=g_recv.at[rel],
            device_id={"space": flip(me, 1)},
            device_id_type=pl.DeviceIdType.MESH,
        ).wait_recv()

    pass_on(0, 2)
    pass_on(0, 4)
    for j in range(1, depth):
        pass_on(0, 8 * j)
    pass_on(0, 1)
    for j in range(depth):
        if j:
            await_block(8 * j)
            pass_on(8 * j, 2)
            pass_on(8 * j, 4)
            pass_on(8 * j, 1)
        if j == 0:
            for near in (2, 4):
                await_block(near)
                if (near == 4) == (j in forks):
                    pass_on(near, 6 - near)
                pass_on(near, 1)
    margin = (banded_ref.shape[0] - high_rows) // 2
    group = count // depth
    span = group * two

    def lat_step(d):
        at = pl.multiple_of(d * span, 16)
        fields = [
            whole_ref[pl.ds(d * group, group), :, tile_cols(t)].reshape(span, LANES)
            for t in range(lane_tiles)
        ]
        products = [
            [mem_ref[m, t, pl.ds(at, span), :] * fields[t] for t in range(lane_tiles)]
            for m in range(members)
        ]
        sides = [
            jnp.dot(
                jnp.concatenate(
                    [jnp.concatenate(p[side : side + 2], axis=1) for p in products], axis=0
                ),
                lat_ref[side],
                preferred_element_type=jnp.float32,
            )
            for side in range(2)
        ]
        bands = [
            sides[0][:, :LANES],
            sides[0][:, LANES:] + sides[1][:, :LANES],
            sides[1][:, LANES:],
        ]
        for t, band in enumerate(bands):
            narrow = band.astype(jnp.bfloat16)
            for m in range(members):
                banded_ref[pl.ds(at + margin, span), tile_cols(t * members + m)] = narrow[
                    m * span : (m + 1) * span
                ]

    def near_blocks(j):
        for near in (2, 4):
            rel = 8 * j + near
            await_block(rel)
            if (near == 4) == (j in forks):
                pass_on(rel, 6 - near)
            pass_on(rel, 1)

    for copy in mem_loads:
        copy.wait()
    def finish(j):
        await_block(8 * j + 6)
        pass_on(8 * j + 6, 1)

    def band(j):
        for column in range(1, 8, 2):
            await_block(8 * j + column)
        lat_step(flip_all(me, 8 * j) // 8)

    lead = min(1, depth - 1)
    for j in range(1, depth):
        near_blocks(j)
    for j in range(depth + lead):
        if j < depth:
            finish(j)
        if j >= lead:
            band(j - lead)

    banded_ref[:margin] = banded_ref[high_rows : high_rows + margin]
    banded_ref[high_rows + margin :] = banded_ref[margin : 2 * margin]

    band_rows, band_depth = lon_ref.shape
    inset = margin - (band_depth - band_rows) // 2

    def lon_step(q, carry):
        at = pl.multiple_of(q * band_rows, 16)
        for t in range(lane_tiles):
            total = jnp.zeros((band_rows, LANES), jnp.float32)
            for m in range(0, members, 2):
                start = (t * members + m) * LANES
                spread = jnp.dot(
                    lon_ref[...],
                    banded_ref[pl.ds(at + inset, band_depth), start : start + 2 * LANES],
                    preferred_element_type=jnp.float32,
                )
                for k in range(2):
                    total += (
                        mem_ref[m + k, t, pl.ds(at, band_rows), :].astype(jnp.float32)
                        * spread[:, tile_cols(k)]
                    )
            contrib_ref[pl.ds(at + 8, band_rows), tile_cols(t)] = total
        return carry

    def lon_plane(p):
        per = span // band_rows
        lax.fori_loop(p * per, (p + 1) * per, lon_step, 0)

    for p in range(depth):
        at = p * span
        ahead = (at - 8) % high_rows
        for t in range(lane_tiles):
            total = jnp.zeros((16, LANES), jnp.float32)
            for m in range(0, members, 2):
                start = (t * members + m) * LANES
                spread = jnp.dot(
                    rim_ref[...],
                    banded_ref[at : at + 2 * margin, start : start + 2 * LANES],
                    preferred_element_type=jnp.float32,
                )
                for k in range(2):
                    near = jnp.concatenate(
                        [
                            mem_ref[m + k, t, ahead : ahead + 8, :].astype(jnp.float32),
                            mem_ref[m + k, t, at : at + 8, :].astype(jnp.float32),
                        ],
                        axis=0,
                    )
                    total += near * spread[:, tile_cols(k)]
            contrib_ref[at : at + 16, tile_cols(t)] = total
            if p == 0:
                contrib_ref[high_rows + 8 :, tile_cols(t)] = total[8:]

    for copy in sends:
        copy.wait_send()

    def part_of(rel):
        at = pl.multiple_of(flip_all(me, rel) * two, 16)
        body = contrib_ref[pl.ds(at + 8, two), :]
        ahead = contrib_ref[pl.ds(at, 8), :]
        behind = contrib_ref[pl.ds(at + 8 + two, 8), :]
        row = lax.broadcasted_iota(jnp.int32, (8, lats), 0)
        return body, jnp.where(row < 4, behind, ahead)

    reduce_sends = []

    def ship(value, slot, stride):
        out_buf[slot, :two] = value[0].astype(jnp.bfloat16)
        out_buf[slot, two:] = value[1].astype(jnp.bfloat16)
        copy = pltpu.make_async_remote_copy(
            src_ref=out_buf.at[slot],
            dst_ref=in_buf.at[slot],
            send_sem=r_send.at[slot],
            recv_sem=r_recv.at[slot],
            device_id={"space": flip_all(me, stride)},
            device_id_type=pl.DeviceIdType.MESH,
        )
        copy.start()
        reduce_sends.append(copy)
        return copy

    flying = {}

    def arrived(value, slot):
        flying[slot].wait_recv()
        return (
            value[0] + in_buf[slot, :two].astype(jnp.float32),
            value[1] + in_buf[slot, two:].astype(jnp.float32),
        )

    column_of = {6: 0, 2: 1, 4: 2, 0: 3}
    far = list(range(depth))[::-1]
    base = 4 * depth
    last = base + 3 * depth

    def to_partner(j):
        lon_plane(flip_all(me, 8 * j) // 8)
        for column in (6, 2, 4, 0):
            slot = column_of[column] * depth + j
            flying[slot] = ship(part_of(8 * j + column + 1), slot, 1)

    def chip_part(column, j):
        return arrived(part_of(8 * j + column), column_of[column] * depth + j)

    def to_sides(j):
        for column, slot in ((6, base), (2, base + depth), (4, base + 2 * depth)):
            flying[slot + j] = ship(chip_part(column, j), slot + j, column)

    def column_sum(j):
        value = chip_part(0, j)
        for side in range(3):
            value = arrived(value, base + side * depth + j)
        return value

    def along(j):
        if j:
            flying[last + j] = ship(column_sum(j), last + j, 8 * j)

    for place, j in enumerate(far):
        to_partner(j)
        if place:
            to_sides(far[place - 1])
    to_sides(0)
    for j in far:
        along(j)
    value = column_sum(0)
    for j in range(1, depth):
        value = arrived(value, last + j)
    body = value[0] / (total_members - 1.0)
    rim = value[1] / (total_members - 1.0)
    for t in range(lane_tiles):
        total_ref[t, 0:8, :] = rim[:, tile_cols(t)]
        total_ref[t, 8 : 8 + two, :] = body[:, tile_cols(t)]
        total_ref[t, 8 + two :, :] = rim[:, tile_cols(t)]
        stage_ref[0, t] = body[:, tile_cols(t)]
    wide = rows + 4
    for c in range(var_count):
        values = tile_rows(total_ref, pl.ds(4 + c, wide, stride=var_count))
        for b in range(3):
            moved = shifted(values, b)
            for t in range(lane_tiles):
                taps_ref[0, t, pl.ds(2 * b + c, wide, stride=8), :] = moved[:, tile_cols(t)]

    def tail_pair(p):
        for chunk in lane_chunks():
            lines = [(2 * p + line, t) for line, t in chunk]
            field = jnp.concatenate([tap_block(0, j, t) for j, t in lines], axis=1)
            tangent = jnp.dot(
                w_tail[...], field.astype(jnp.bfloat16), preferred_element_type=jnp.float32
            )
            slopes = jnp.concatenate([slopes_ref[j, :, tile_cols(t)] for j, t in lines], axis=1)
            back = (slopes * tangent).astype(jnp.bfloat16)
            for place, (j, t) in enumerate(lines):
                back_ref[j, :hidden, tile_cols(t)] = back[:, tile_cols(place)]

    in_groups(tail_pair, 0, pairs, TAIL_GROUP)
    in_groups(functools.partial(project_pair, v_tail[...]), 0, pairs, TAIL_GROUP)
    gather_pieces()
    for c in range(var_count):
        values = tile_rows(total_ref, pl.ds(8 + c, rows, stride=var_count)) + assembled(c)
        for t in range(lane_tiles):
            stage_ref[1, t, pl.ds(c, rows, stride=var_count), :] = values[:, tile_cols(t)]
    for copy in reduce_sends:
        copy.wait_send()


def emit_kernel(tiled_ref, incr_hbm, resp_hbm, out_sem):
    _, tiles, two, _ = tiled_ref.shape
    stores = []
    for index, target in enumerate((incr_hbm, resp_hbm)):
        for t in range(tiles):
            copy = pltpu.make_async_copy(
                tiled_ref.at[index, t],
                target.reshape(two, tiles * LANES).at[:, tile_cols(t)],
                out_sem.at[index, t],
            )
            copy.start()
            stores.append(copy)
    for copy in stores:
        copy.wait()


def whole_step(members, state, cotangent, conv_in, conv_out, bias):
    count = lax.axis_size("space")
    mine, lons, var_count, lats = members.shape
    rows = state.shape[0]
    hidden = bias.shape[0]
    two = rows * var_count
    tiles = lats // LANES
    depth = count // 8
    any_space = pl.BlockSpec(memory_space=pl.ANY)
    vmem = pltpu.VMEM
    dma = pltpu.SemaphoreType.DMA
    margin = HALF * var_count
    window = lats - LANES
    slots = 8 * depth
    tiled = pl.pallas_call(
        functools.partial(step_kernel, count, mine * count),
        out_shape=jax.ShapeDtypeStruct((2, tiles, two, LANES), jnp.float32),
        in_specs=[any_space] * 6,
        out_specs=pl.BlockSpec(memory_space=vmem),
        scratch_shapes=[
            vmem((mine, tiles, lons * var_count, LANES), jnp.bfloat16),
            vmem((2, tiles, two, LANES), jnp.float32),
            vmem((2, 2, tiles, 8, LANES), jnp.float32),
            vmem((2, tiles, (rows + 5) * 8, LANES), jnp.float32),
            vmem((2, 3, 3, var_count, hidden), jnp.float32),
            vmem((1, hidden), jnp.float32),
            vmem((4, 32, hidden), jnp.float32),
            vmem((hidden, 96), jnp.bfloat16),
            vmem((hidden, 96), jnp.bfloat16),
            vmem((64, 2 * hidden), jnp.bfloat16),
            vmem((hidden, 32), jnp.bfloat16),
            vmem((32, hidden), jnp.bfloat16),
            vmem((rows + 2, hidden, lats), jnp.float32),
            vmem((rows + 2, 2 * hidden, lats), jnp.bfloat16),
            vmem((rows + 2, 24, lats), jnp.float32),
            vmem((tiles, rows * 8, LANES), jnp.float32),
            vmem((tiles, two, LANES), jnp.float32),
            vmem((count, two, lats), jnp.bfloat16),
            vmem((2, window, window), jnp.bfloat16),
            vmem((4 * two, 4 * two + 2 * margin), jnp.bfloat16),
            vmem((16, 2 * (margin + 16)), jnp.bfloat16),
            vmem((lons * var_count + 2 * (margin + 16), mine * lats), jnp.bfloat16),
            vmem((lons * var_count + 16, lats), jnp.float32),
            vmem((slots, two + 8, lats), jnp.bfloat16),
            vmem((slots, two + 8, lats), jnp.bfloat16),
            vmem((tiles, two + 16, LANES), jnp.float32),
            dma((mine, tiles)),
            dma((2, tiles)),
            dma((3,)),
            dma((2,)),
            dma((2,)),
            dma((count,)),
            dma((count,)),
            dma((slots,)),
            dma((slots,)),
        ],
        compiler_params=pltpu.CompilerParams(collective_id=2, has_side_effects=True),
        name="whole_step",
    )(
        members,
        state,
        cotangent,
        jnp.transpose(conv_in, (0, 1, 3, 2)),
        conv_out,
        bias.reshape(1, hidden),
    )
    return pl.pallas_call(
        emit_kernel,
        out_shape=(jax.ShapeDtypeStruct(state.shape, jnp.float32),) * 2,
        in_specs=[pl.BlockSpec(memory_space=vmem)],
        out_specs=(any_space,) * 2,
        scratch_shapes=[dma((2, tiles))],
        name="emit",
    )(tiled)


def fits(members, state, bias):
    count = lax.axis_size("space")
    mine, lons, var_count, lats = members.shape
    rows = state.shape[0]
    return (
        lax.axis_size("mem") == 1
        and count >= 8
        and count & (count - 1) == 0
        and var_count == 2
        and lats == 3 * LANES
        and rows % 8 == 0
        and rows >= 2 * 8
        and mine % 2 == 0
        and lons == count * rows
        and bias.shape[0] == LANES
    )


def per_device(members, state, cotangent, conv_in, conv_out, bias):
    row_count, var_count, lat_count = state.shape
    if fits(members, state, bias):
        return whole_step(members, state, cotangent, conv_in, conv_out, bias)
    count = lax.axis_size("space")
    direct = count >= 8 and count & (count - 1) == 0
    rim_width = 2
    joined = jnp.concatenate([state, cotangent], axis=1)
    padded = padded_2(joined, "space", rim_width)
    state_pad = padded[:, :var_count]
    cot_pad = padded[:, var_count:]
    activity = jnp.tanh(convolve_fine(state_pad, conv_in) + bias[None, :, None])
    slopes = 1.0 - activity * activity
    backward = slopes * convolve_fine(cot_pad, flipped(conv_out))
    gradient = cotangent + convolve_fine(backward, flipped(conv_in))
    gradient = gradient.astype(jnp.bfloat16)
    width = var_count * lat_count
    gradient = gradient.reshape(row_count, width)
    if direct:
        whole = gather(gradient).reshape(count * row_count, width)
    else:
        whole = lax.all_gather(gradient, "space", axis=0, tiled=True)
    merged = members.reshape(members.shape[0], members.shape[1], width)
    lat_loc = band_matrix(lat_count, False)
    lon_loc = band_matrix(merged.shape[1], True)
    contrib = covariance(merged, whole, lat_loc, lon_loc)
    member_count = members.shape[0] * lax.axis_size("space") * lax.axis_size("mem")
    if direct:
        own, left, right = scatter(
            contrib.reshape(count, row_count, width), rim_width
        )
        total = jnp.concatenate([left, own, right], axis=0)
        total = total.reshape(row_count + 2 * rim_width, var_count, lat_count)
        if lax.axis_size("mem") > 1:
            total = lax.psum(total, "mem")
        incr_pad = total / (member_count - 1.0)
        increment = incr_pad[rim_width : rim_width + row_count]
    else:
        member_sum = lax.psum(contrib, "mem")
        block_sum = lax.psum_scatter(member_sum, "space", scatter_dimension=0, tiled=True)
        increment = block_sum.reshape(state.shape) / (member_count - 1.0)
        incr_pad = padded_2(increment, "space", rim_width)
    tangent_hidden = slopes * convolve(incr_pad, conv_in)
    response = increment + convolve(tangent_hidden, conv_out)
    return (increment, response)


def solution(mesh):
    in_specs = (
        P(("space", "mem"), None, None, None),
        P("space", None, None),
        P("space", None, None),
        P(),
        P(),
        P(),
    )
    out_specs = (P("space", None, None), P("space", None, None))
    return jax.shard_map(
        per_device, mesh=mesh, in_specs=in_specs, out_specs=out_specs, check_vma=False
    )
```

```python
import functools

import jax
import jax.numpy as jnp
from jax import lax
from jax.experimental import pallas as pl
from jax.experimental.pallas import tpu as pltpu
from jax.sharding import PartitionSpec as P

HALF = 16
LANES = 128
HEAD_GROUP = 11
TAIL_GROUP = 13


def flip(index, stride):
    return index + stride * (1 - 2 * lax.rem(index // stride, 2))


def flip_all(index, mask):
    stride = 1
    while stride <= mask:
        if mask & stride:
            index = flip(index, stride)
        stride *= 2
    return index


def stages_of(count):
    held = [0]
    steps = []
    stride = count // 2
    while stride >= 8:
        steps.append([(stride, list(held))])
        held = held + [m ^ stride for m in held]
        stride //= 2
    half = max(1, len(held) // 2)
    first, second = held[:half], held[half:]
    steps.append([(2, first), (4, second)])
    first = first + [m ^ 2 for m in first]
    second = second + [m ^ 4 for m in second]
    steps.append([(4, first), (2, second)])
    return steps


def greet(me, count, extra=()):
    barrier = pltpu.get_barrier_semaphore()
    friends = list(extra)
    stride = 1
    while stride < count:
        friends.append(flip(me, stride))
        stride *= 2
    for friend in friends:
        pl.semaphore_signal(
            barrier, inc=1, device_id={"space": friend}, device_id_type=pl.DeviceIdType.MESH
        )
    pl.semaphore_wait(barrier, len(friends))


def gather_kernel(count, block_ref, whole_ref, send_sem, recv_sem):
    me = lax.axis_index("space")
    greet(me, count)

    def remote(mask, stride):
        owner = flip_all(me, mask)
        source = block_ref if mask == 0 else whole_ref.at[owner]
        slot = mask ^ stride
        return pltpu.make_async_remote_copy(
            src_ref=source,
            dst_ref=whole_ref.at[owner],
            send_sem=send_sem.at[slot],
            recv_sem=recv_sem.at[slot],
            device_id={"space": flip(me, stride)},
            device_id_type=pl.DeviceIdType.MESH,
        )

    started = []
    pair = []
    for step in stages_of(count):
        now = []
        for position in range(max(len(masks) for stride, masks in step)):
            for stride, masks in step:
                if position < len(masks):
                    copy = remote(masks[position], stride)
                    copy.start()
                    now.append((copy, masks[position] ^ stride))
        if not pair:
            copy = remote(0, 1)
            copy.start()
            pair.append(copy)
            whole_ref[me] = block_ref[...]
        for copy, mask in now:
            copy.wait_recv()
            other = remote(mask, 1)
            other.start()
            pair.append(other)
            started.append(copy)
    for copy in started:
        copy.wait_send()
    for copy in pair:
        copy.wait()


def gather(block):
    count = lax.axis_size("space")
    return pl.pallas_call(
        functools.partial(gather_kernel, count),
        out_shape=jax.ShapeDtypeStruct((count,) + block.shape, block.dtype),
        in_specs=[pl.BlockSpec(memory_space=pltpu.VMEM)],
        out_specs=pl.BlockSpec(memory_space=pltpu.VMEM),
        scratch_shapes=[
            pltpu.SemaphoreType.DMA((count,)),
            pltpu.SemaphoreType.DMA((count,)),
        ],
        compiler_params=pltpu.CompilerParams(collective_id=0, has_side_effects=True),
        name="gather",
    )(block)


def scatter_kernel(
    count, rim, part_ref, sum_ref, left_ref, right_ref,
    out_buf, in_buf, edge_buf, send_sem, recv_sem, edge_send, edge_recv,
):
    me = lax.axis_index("space")
    before, after = lax.rem(me + count - 1, count), lax.rem(me + 1, count)
    greet(me, count, (before, after))
    arrived = {mask: [] for mask in range(count)}

    def value(mask):
        total = part_ref[flip_all(me, mask)]
        for slot in arrived[mask]:
            total = total + in_buf[slot].astype(jnp.float32)
        return total

    sent = []
    for step in [[(1, list(range(0, count, 2)))]] + stages_of(count)[::-1]:
        now = []
        for position in range(max(len(masks) for stride, masks in step)):
            for stride, masks in step:
                if position < len(masks):
                    slot = masks[position] ^ stride
                    out_buf[slot] = value(slot).astype(out_buf.dtype)
                    copy = pltpu.make_async_remote_copy(
                        src_ref=out_buf.at[slot],
                        dst_ref=in_buf.at[slot],
                        send_sem=send_sem.at[slot],
                        recv_sem=recv_sem.at[slot],
                        device_id={"space": flip(me, stride)},
                        device_id_type=pl.DeviceIdType.MESH,
                    )
                    copy.start()
                    now.append((copy, masks[position], slot))
        for copy, mask, slot in now:
            copy.wait_recv()
            arrived[mask].append(slot)
            sent.append(copy)
    total = value(0)
    sum_ref[...] = total
    edge_buf[0] = total[:rim]
    edge_buf[1] = total[total.shape[0] - rim :]
    edges = [
        pltpu.make_async_remote_copy(
            src_ref=edge_buf.at[side],
            dst_ref=target,
            send_sem=edge_send.at[side],
            recv_sem=edge_recv.at[side],
            device_id={"space": friend},
            device_id_type=pl.DeviceIdType.MESH,
        )
        for side, target, friend in ((0, right_ref, before), (1, left_ref, after))
    ]
    for copy in edges:
        copy.start()
    for copy in sent:
        copy.wait_send()
    for copy in edges:
        copy.wait()


def scatter(parts, rim):
    count, rows, lat_count = parts.shape
    return pl.pallas_call(
        functools.partial(scatter_kernel, count, rim),
        out_shape=(
            jax.ShapeDtypeStruct((rows, lat_count), jnp.float32),
            jax.ShapeDtypeStruct((rim, lat_count), jnp.float32),
            jax.ShapeDtypeStruct((rim, lat_count), jnp.float32),
        ),
        in_specs=[pl.BlockSpec(memory_space=pltpu.VMEM)],
        out_specs=(pl.BlockSpec(memory_space=pltpu.VMEM),) * 3,
        scratch_shapes=[
            pltpu.VMEM((count, rows, lat_count), jnp.bfloat16),
            pltpu.VMEM((count, rows, lat_count), jnp.bfloat16),
            pltpu.VMEM((2, rim, lat_count), jnp.float32),
            pltpu.SemaphoreType.DMA((count,)),
            pltpu.SemaphoreType.DMA((count,)),
            pltpu.SemaphoreType.DMA((2,)),
            pltpu.SemaphoreType.DMA((2,)),
        ],
        compiler_params=pltpu.CompilerParams(collective_id=1, has_side_effects=True),
        name="scatter",
    )(parts)


def covariance_kernel(members_ref, whole_ref, lat_ref, lon_ref, sum_ref, banded_ref):
    lat_count = lat_ref.shape[0]

    @pl.when(pl.program_id(0) == 0)
    def _():
        sum_ref[...] = jnp.zeros_like(sum_ref)

    for start in range(0, whole_ref.shape[1], lat_count):
        columns = slice(start, start + lat_count)
        product = members_ref[0, :, columns].astype(jnp.float32) * whole_ref[:, columns].astype(
            jnp.float32
        )
        banded_ref[:, columns] = jnp.dot(
            product.astype(jnp.bfloat16), lat_ref[...], preferred_element_type=jnp.float32
        ).astype(jnp.bfloat16)
    for start in range(0, whole_ref.shape[1], lat_count):
        columns = slice(start, start + lat_count)
        spread = jnp.dot(
            lon_ref[...], banded_ref[:, columns], preferred_element_type=jnp.float32
        )
        sum_ref[:, columns] += members_ref[0, :, columns].astype(jnp.float32) * spread


def covariance(members, whole, lat_loc, lon_loc):
    count, lon_count, width = members.shape
    return pl.pallas_call(
        covariance_kernel,
        grid=(count,),
        out_shape=jax.ShapeDtypeStruct((lon_count, width), jnp.float32),
        in_specs=[
            pl.BlockSpec((1, lon_count, width), lambda m: (m, 0, 0)),
            pl.BlockSpec(whole.shape, lambda m: (0, 0)),
            pl.BlockSpec(lat_loc.shape, lambda m: (0, 0)),
            pl.BlockSpec(lon_loc.shape, lambda m: (0, 0)),
        ],
        out_specs=pl.BlockSpec((lon_count, width), lambda m: (0, 0)),
        scratch_shapes=[pltpu.VMEM((lon_count, width), jnp.bfloat16)],
        name="covariance",
    )(members, whole, lat_loc, lon_loc)


def padded_2(cells, axis, width):
    count = lax.axis_size(axis)
    head = cells[:width]
    tail = cells[cells.shape[0] - width :]
    return jnp.concatenate(
        [
            lax.ppermute(tail, axis, [(i, (i + 1) % count) for i in range(count)]),
            cells,
            lax.ppermute(head, axis, [((i + 1) % count, i) for i in range(count)]),
        ],
        axis=0,
    )


def convolve(padded, weight, precision=None):
    row_count = padded.shape[0] - 2
    lat_count = padded.shape[2]
    out_count = weight.shape[2]
    in_count = weight.shape[3]
    if precision is None:
        padded = padded.astype(jnp.bfloat16)
        weight = weight.astype(jnp.bfloat16)
    if out_count <= in_count:
        flattened = weight.reshape(9 * out_count, in_count)
        product = jnp.einsum(
            "kc,xcy->xky", flattened, padded, preferred_element_type=jnp.float32
        )
        product = jnp.pad(product, ((0, 0), (0, 0), (1, 1)))
        summed = jnp.zeros((row_count, out_count, lat_count), jnp.float32)
        for step_lon in range(3):
            for step_lat in range(3):
                tap_index = step_lon * 3 + step_lat
                summed = (
                    summed
                    + product[
                        step_lon : step_lon + row_count,
                        tap_index * out_count : (tap_index + 1) * out_count,
                        step_lat : step_lat + lat_count,
                    ]
                )
        return summed
    lat_padded = jnp.pad(padded, ((0, 0), (0, 0), (1, 1)))
    stacked = jnp.concatenate(
        [
            lat_padded[step_lon : step_lon + row_count, :, step_lat : step_lat + lat_count]
            for step_lon in range(3)
            for step_lat in range(3)
        ],
        axis=1,
    )
    flattened = jnp.transpose(weight, (2, 0, 1, 3)).reshape(out_count, 9 * in_count)
    return jnp.einsum(
        "ok,xky->xoy", flattened, stacked, precision=precision, preferred_element_type=jnp.float32
    )


def split(values):
    high = lax.reduce_precision(values, 8, 7)
    return high.astype(jnp.bfloat16), (values - high).astype(jnp.bfloat16)


def convolve_fine(padded, weight):
    out_count, in_count = weight.shape[2:]
    upper, lower = split(padded)
    weight_upper, weight_lower = split(weight)
    if out_count <= in_count:
        both = jnp.concatenate([upper, lower], axis=1)
        stacked = jnp.concatenate([weight_upper, weight_lower], axis=2)
        stacked = jnp.concatenate([stacked, stacked], axis=3)
        result = convolve(both, stacked)
        return result[:, :out_count] + result[:, out_count:]
    return convolve(padded, weight, lax.Precision.HIGH)


def flipped(weight):
    return jnp.transpose(weight[::-1, ::-1], (0, 1, 3, 2))


def band_matrix(count, wrap):
    row_index = jnp.arange(count)[:, None]
    col_index = jnp.arange(count)[None, :]
    distance = jnp.abs(row_index - col_index)
    if wrap:
        distance = jnp.minimum(distance, count - distance)
    ratio = distance.astype(jnp.float32) / (HALF + 1.0)
    return jnp.where(distance <= HALF, 1.0 - ratio * ratio, 0.0).astype(jnp.bfloat16)


def tile_cols(t):
    return slice(t * LANES, (t + 1) * LANES)


def shifted(values, step):
    if step == 1:
        return values
    width = values.shape[-1]
    column = lax.broadcasted_iota(jnp.int32, values.shape, values.ndim - 1)
    if step == 0:
        return jnp.where(column == 0, 0.0, pltpu.roll(values, 1, values.ndim - 1))
    return jnp.where(column == width - 1, 0.0, pltpu.roll(values, width - 1, values.ndim - 1))


def tap_of(distance):
    ratio = distance / (HALF + 1.0)
    return jnp.where(distance <= HALF, 1.0 - ratio * ratio, 0.0)


def halves(values):
    high = values.astype(jnp.bfloat16)
    return high, (values - high.astype(jnp.float32)).astype(jnp.bfloat16)


def step_kernel(
    count, total_members,
    members_hbm, state_hbm, cot_hbm, win_hbm, wout_hbm, bias_hbm,
    stage_ref,
    mem_ref, own_ref, halo_ref, taps_ref, wraw_ref, bias_ref, slot_ref,
    w_state, w_cot, v_in, w_tail, v_tail,
    slopes_ref, back_ref, part_ref, q_ref, g_ref, whole_ref, lat_ref, lon_ref, rim_ref, banded_ref, contrib_ref,
    out_buf, in_buf, total_ref,
    mem_sem, own_sem, small_sem, halo_send, halo_recv, g_send, g_recv, r_send, r_recv,
):
    me = lax.axis_index("space")
    members, lane_tiles, high_rows, _ = mem_ref.shape
    var_count = wraw_ref.shape[3]
    two = own_ref.shape[2]
    rows = two // var_count
    lats = lane_tiles * LANES
    hidden = slot_ref.shape[2]
    depth = count // 8
    before, after = lax.rem(me + count - 1, count), lax.rem(me + 1, count)

    own_loads = []
    for index, source in enumerate((state_hbm, cot_hbm)):
        for t in range(lane_tiles):
            copy = pltpu.make_async_copy(
                source.reshape(two, lats).at[:, tile_cols(t)],
                own_ref.at[index, t],
                own_sem.at[index, t],
            )
            copy.start()
            own_loads.append(copy)
    small_loads = [
        pltpu.make_async_copy(win_hbm, wraw_ref.at[0], small_sem.at[0]),
        pltpu.make_async_copy(wout_hbm, wraw_ref.at[1], small_sem.at[1]),
        pltpu.make_async_copy(bias_hbm, bias_ref, small_sem.at[2]),
    ]
    for copy in small_loads:
        copy.start()
    mem_loads = []
    flat_members = members_hbm.reshape(members, high_rows, lats)
    for m in range(members):
        for t in range(lane_tiles):
            copy = pltpu.make_async_copy(
                flat_members.at[m, :, tile_cols(t)], mem_ref.at[m, t], mem_sem.at[m, t]
            )
            copy.start()
            mem_loads.append(copy)

    barrier = pltpu.get_barrier_semaphore()
    friends = [before, after, flip(me, 1), flip(me, 2), flip(me, 4), flip_all(me, 6)]
    friends += [flip_all(me, 8 * j) for j in range(1, depth)]
    for friend in friends:
        pl.semaphore_signal(
            barrier, inc=1, device_id={"space": friend}, device_id_type=pl.DeviceIdType.MESH
        )

    row = lax.broadcasted_iota(jnp.int32, taps_ref.shape[2:], 0)
    blank = jnp.where((row & 7) == 6, 1.0, 0.0)
    for index in range(2):
        for t in range(lane_tiles):
            taps_ref[index, t] = blank
    window = lat_ref.shape[1]
    for index in range(2):
        offset = index * (lats - window)
        y = lax.broadcasted_iota(jnp.int32, (window, window), 0)
        z = lax.broadcasted_iota(jnp.int32, (window, window), 1)
        value = tap_of(jnp.abs(y - z).astype(jnp.float32))
        mine = (z + offset < lats // 2) if index == 0 else (z + offset >= lats // 2)
        lat_ref[index] = jnp.where(mine, value, 0.0).astype(jnp.bfloat16)
    i = lax.broadcasted_iota(jnp.int32, lon_ref.shape, 0)
    j = lax.broadcasted_iota(jnp.int32, lon_ref.shape, 1)
    gap = i - j + var_count * HALF
    value = tap_of(jnp.abs(gap).astype(jnp.float32) * 0.5)
    lon_ref[...] = jnp.where((gap & 1) == 0, value, 0.0).astype(jnp.bfloat16)
    i = lax.broadcasted_iota(jnp.int32, rim_ref.shape, 0)
    j = lax.broadcasted_iota(jnp.int32, rim_ref.shape, 1)
    gap = i - j + rim_ref.shape[1] // 2 - 8
    value = tap_of(jnp.abs(gap).astype(jnp.float32) * 0.5)
    rim_ref[...] = jnp.where((gap & 1) == 0, value, 0.0).astype(jnp.bfloat16)

    for copy in small_loads:
        copy.wait()
    slot_ref[...] = jnp.zeros(slot_ref.shape, jnp.float32)
    for a in range(3):
        for b in range(3):
            place = slice(8 * a + 2 * b, 8 * a + 2 * b + 2)
            slot_ref[0, place, :] = wraw_ref[0, a, b]
            slot_ref[1, place, :] = wraw_ref[0, 2 - a, 2 - b]
            slot_ref[2, place, :] = wraw_ref[1, 2 - a, 2 - b]
            slot_ref[3, place, :] = wraw_ref[1, a, b]
    w_tail[...] = slot_ref[0].T.astype(jnp.bfloat16)
    v_tail[...] = slot_ref[3].astype(jnp.bfloat16)
    slot_ref[0, 14:15, :] = bias_ref[...]
    for target, index in ((w_state, 0), (w_cot, 2)):
        high, low = halves(slot_ref[index].T)
        target[...] = jnp.concatenate([high, high, low], axis=1)
    high, low = halves(slot_ref[1])
    v_in[:32] = jnp.concatenate([high, high], axis=1)
    v_in[32:] = jnp.concatenate([low, low], axis=1)

    for copy in own_loads:
        copy.wait()
    pl.semaphore_wait(barrier, len(friends))
    edges = []
    for side, start, friend in ((1, 0, before), (0, two - 8, after)):
        copy = pltpu.make_async_remote_copy(
            src_ref=own_ref.at[:, :, start : start + 8],
            dst_ref=halo_ref.at[side],
            send_sem=halo_send.at[side],
            recv_sem=halo_recv.at[side],
            device_id={"space": friend},
            device_id_type=pl.DeviceIdType.MESH,
        )
        copy.start()
        edges.append(copy)

    for index in range(2):
        for c in range(var_count):
            values = jnp.concatenate(
                [own_ref[index, t, pl.ds(c, rows, stride=var_count), :] for t in range(lane_tiles)],
                axis=1,
            )
            for b in range(3):
                moved = shifted(values, b)
                for t in range(lane_tiles):
                    taps_ref[index, t, pl.ds(16 + 2 * b + c, rows, stride=8), :] = moved[:, tile_cols(t)]

    def lane_chunks():
        tiles = [(line, t) for line in range(2) for t in range(lane_tiles)]
        return [tiles[k : k + 2] for k in range(0, len(tiles), 2)]

    def tap_block(index, j, t):
        start = 8 * j if isinstance(j, int) else pl.multiple_of(8 * j, 8)
        return taps_ref[index, t, pl.ds(start, 32), :]

    def fine_block(index, j, t):
        high, low = halves(tap_block(index, j, t))
        return jnp.concatenate([high, low, high], axis=0)

    def in_groups(step, first, last, group):
        def several(k, carry):
            for place in range(group):
                step(first + k * group + place)
            return carry

        full = (last - first) // group
        lax.fori_loop(0, full, several, 0)
        for p in range(first + full * group, last):
            step(p)

    def head_pair(p):
        for chunk in lane_chunks():
            lines = [(2 * p + line, t) for line, t in chunk]
            field = jnp.concatenate([fine_block(0, j, t) for j, t in lines], axis=1)
            misfit = jnp.concatenate([fine_block(1, j, t) for j, t in lines], axis=1)
            activity = jnp.tanh(jnp.dot(w_state[...], field, preferred_element_type=jnp.float32))
            slopes = 1.0 - activity * activity
            back = slopes * jnp.dot(w_cot[...], misfit, preferred_element_type=jnp.float32)
            back = jnp.concatenate(halves(back), axis=0)
            for place, (j, t) in enumerate(lines):
                slopes_ref[j, :, tile_cols(t)] = slopes[:, tile_cols(place)]
                back_ref[j, :, tile_cols(t)] = back[:, tile_cols(place)]

    def project_pair(weights, p):
        for chunk in lane_chunks():
            lines = [(2 * p + line, t) for line, t in chunk]
            pieces = jnp.dot(
                weights,
                jnp.concatenate(
                    [back_ref[j, : weights.shape[1], tile_cols(t)] for j, t in lines], axis=1
                ),
                preferred_element_type=jnp.float32,
            )
            if pieces.shape[0] > 32:
                pieces = pieces[:32] + pieces[32:]
            for place, (j, t) in enumerate(lines):
                part_ref[j, :, tile_cols(t)] = pieces[:24, tile_cols(place)]

    pairs = (rows + 2) // 2

    in_groups(head_pair, 1, pairs - 1, HEAD_GROUP)
    in_groups(functools.partial(project_pair, v_in[...]), 1, pairs - 1, HEAD_GROUP)

    for copy in edges:
        copy.wait()
    for side, slot, first in ((0, 0, 4), (1, rows + 2, 0)):
        for index in range(2):
            values = jnp.concatenate(
                [halo_ref[side, index, t] for t in range(lane_tiles)], axis=1
            )
            for b in range(3):
                moved = shifted(values, b)
                for line in range(2):
                    at = 8 * (slot + line) + 2 * b
                    for t in range(lane_tiles):
                        taps_ref[index, t, at : at + 2, :] = moved[
                            first + 2 * line : first + 2 * line + 2, tile_cols(t)
                        ]

    for p in (0, pairs - 1):
        head_pair(p)
    for p in (0, pairs - 1):
        project_pair(v_in[...], p)

    def assembled(c):
        return sum(
            shifted(tile_rows(q_ref, pl.ds(2 * b + c, rows, stride=8)), b) for b in range(3)
        )

    def tile_rows(ref, place):
        return jnp.concatenate([ref[t, place, :] for t in range(lane_tiles)], axis=1)

    def gather_pieces():
        for t in range(lane_tiles):
            cols = tile_cols(t)
            joined = (
                part_ref[0:rows, 0:8, cols]
                + part_ref[1 : rows + 1, 8:16, cols]
                + part_ref[2 : rows + 2, 16:24, cols]
            )
            q_ref[t] = joined.reshape(rows * 8, LANES)

    gather_pieces()
    for c in range(var_count):
        values = jnp.concatenate(
            [own_ref[1, t, pl.ds(c, rows, stride=var_count), :] for t in range(lane_tiles)], axis=1
        )
        values = values + assembled(c)
        for t in range(lane_tiles):
            g_ref[t, pl.ds(c, rows, stride=var_count), :] = values[:, tile_cols(t)]
    whole_ref[me] = tile_rows(g_ref, slice(None)).astype(jnp.bfloat16)

    forks = [j for j in range(depth) if bin(j).count("1") % 2 == 0]
    sends = []

    def pass_on(rel, stride):
        owner = flip_all(me, rel)
        slot = rel ^ stride
        copy = pltpu.make_async_remote_copy(
            src_ref=whole_ref.at[owner],
            dst_ref=whole_ref.at[owner],
            send_sem=g_send.at[len(sends)],
            recv_sem=g_recv.at[slot],
            device_id={"space": flip_all(me, stride)},
            device_id_type=pl.DeviceIdType.MESH,
        )
        copy.start()
        sends.append(copy)

    def await_block(rel):
        owner = flip_all(me, rel)
        pltpu.make_async_remote_copy(
            src_ref=whole_ref.at[owner],
            dst_ref=whole_ref.at[owner],
            send_sem=g_send.at[0],
            recv_sem=g_recv.at[rel],
            device_id={"space": flip(me, 1)},
            device_id_type=pl.DeviceIdType.MESH,
        ).wait_recv()

    pass_on(0, 2)
    pass_on(0, 4)
    for j in range(1, depth):
        pass_on(0, 8 * j)
    pass_on(0, 1)
    for j in range(depth):
        if j:
            await_block(8 * j)
            pass_on(8 * j, 2)
            pass_on(8 * j, 4)
            pass_on(8 * j, 1)
        if j == 0:
            for near in (2, 4):
                await_block(near)
                if (near == 4) == (j in forks):
                    pass_on(near, 6 - near)
                pass_on(near, 1)
    margin = (banded_ref.shape[0] - high_rows) // 2
    group = count // depth
    span = group * two

    def lat_step(d):
        at = pl.multiple_of(d * span, 16)
        fields = [
            whole_ref[pl.ds(d * group, group), :, tile_cols(t)].reshape(span, LANES)
            for t in range(lane_tiles)
        ]
        products = [
            [mem_ref[m, t, pl.ds(at, span), :] * fields[t] for t in range(lane_tiles)]
            for m in range(members)
        ]
        sides = [
            jnp.dot(
                jnp.concatenate(
                    [jnp.concatenate(p[side : side + 2], axis=1) for p in products], axis=0
                ),
                lat_ref[side],
                preferred_element_type=jnp.float32,
            )
            for side in range(2)
        ]
        bands = [
            sides[0][:, :LANES],
            sides[0][:, LANES:] + sides[1][:, :LANES],
            sides[1][:, LANES:],
        ]
        for t, band in enumerate(bands):
            narrow = band.astype(jnp.bfloat16)
            for m in range(members):
                banded_ref[pl.ds(at + margin, span), tile_cols(t * members + m)] = narrow[
                    m * span : (m + 1) * span
                ]

    def near_blocks(j):
        for near in (2, 4):
            rel = 8 * j + near
            await_block(rel)
            if (near == 4) == (j in forks):
                pass_on(rel, 6 - near)
            pass_on(rel, 1)

    for copy in mem_loads:
        copy.wait()
    def finish(j):
        await_block(8 * j + 6)
        pass_on(8 * j + 6, 1)

    def band(j):
        for column in range(1, 8, 2):
            await_block(8 * j + column)
        lat_step(flip_all(me, 8 * j) // 8)

    lead = min(2, depth - 1)
    for j in range(1, depth):
        near_blocks(j)
    for j in range(depth + lead):
        if j < depth:
            finish(j)
        if j >= lead:
            band(j - lead)

    banded_ref[:margin] = banded_ref[high_rows : high_rows + margin]
    banded_ref[high_rows + margin :] = banded_ref[margin : 2 * margin]

    band_rows, band_depth = lon_ref.shape
    inset = margin - (band_depth - band_rows) // 2

    def lon_step(q, carry):
        at = pl.multiple_of(q * band_rows, 16)
        for t in range(lane_tiles):
            total = jnp.zeros((band_rows, LANES), jnp.float32)
            for m in range(0, members, 2):
                start = (t * members + m) * LANES
                spread = jnp.dot(
                    lon_ref[...],
                    banded_ref[pl.ds(at + inset, band_depth), start : start + 2 * LANES],
                    preferred_element_type=jnp.float32,
                )
                for k in range(2):
                    total += (
                        mem_ref[m + k, t, pl.ds(at, band_rows), :].astype(jnp.float32)
                        * spread[:, tile_cols(k)]
                    )
            contrib_ref[pl.ds(at + 8, band_rows), tile_cols(t)] = total
        return carry

    def lon_plane(p):
        per = span // band_rows
        lax.fori_loop(p * per, (p + 1) * per, lon_step, 0)

    for p in range(depth):
        at = p * span
        ahead = (at - 8) % high_rows
        for t in range(lane_tiles):
            total = jnp.zeros((16, LANES), jnp.float32)
            for m in range(0, members, 2):
                start = (t * members + m) * LANES
                spread = jnp.dot(
                    rim_ref[...],
                    banded_ref[at : at + 2 * margin, start : start + 2 * LANES],
                    preferred_element_type=jnp.float32,
                )
                for k in range(2):
                    near = jnp.concatenate(
                        [
                            mem_ref[m + k, t, ahead : ahead + 8, :].astype(jnp.float32),
                            mem_ref[m + k, t, at : at + 8, :].astype(jnp.float32),
                        ],
                        axis=0,
                    )
                    total += near * spread[:, tile_cols(k)]
            contrib_ref[at : at + 16, tile_cols(t)] = total
            if p == 0:
                contrib_ref[high_rows + 8 :, tile_cols(t)] = total[8:]

    for copy in sends:
        copy.wait_send()

    def part_of(rel):
        at = pl.multiple_of(flip_all(me, rel) * two, 16)
        body = contrib_ref[pl.ds(at + 8, two), :]
        ahead = contrib_ref[pl.ds(at, 8), :]
        behind = contrib_ref[pl.ds(at + 8 + two, 8), :]
        row = lax.broadcasted_iota(jnp.int32, (8, lats), 0)
        return body, jnp.where(row < 4, behind, ahead)

    reduce_sends = []

    def ship(value, slot, stride):
        out_buf[slot, :two] = value[0].astype(jnp.bfloat16)
        out_buf[slot, two:] = value[1].astype(jnp.bfloat16)
        copy = pltpu.make_async_remote_copy(
            src_ref=out_buf.at[slot],
            dst_ref=in_buf.at[slot],
            send_sem=r_send.at[slot],
            recv_sem=r_recv.at[slot],
            device_id={"space": flip_all(me, stride)},
            device_id_type=pl.DeviceIdType.MESH,
        )
        copy.start()
        reduce_sends.append(copy)
        return copy

    flying = {}

    def arrived(value, slot):
        flying[slot].wait_recv()
        return (
            value[0] + in_buf[slot, :two].astype(jnp.float32),
            value[1] + in_buf[slot, two:].astype(jnp.float32),
        )

    column_of = {6: 0, 2: 1, 4: 2, 0: 3}
    far = list(range(depth))[::-1]
    base = 4 * depth
    last = base + 3 * depth

    def to_partner(j):
        lon_plane(flip_all(me, 8 * j) // 8)
        for column in (6, 2, 4, 0):
            slot = column_of[column] * depth + j
            flying[slot] = ship(part_of(8 * j + column + 1), slot, 1)

    def chip_part(column, j):
        return arrived(part_of(8 * j + column), column_of[column] * depth + j)

    def to_sides(j):
        for column, slot in ((6, base), (2, base + depth), (4, base + 2 * depth)):
            flying[slot + j] = ship(chip_part(column, j), slot + j, column)

    def column_sum(j):
        value = chip_part(0, j)
        for side in range(3):
            value = arrived(value, base + side * depth + j)
        return value

    def along(j):
        if j:
            flying[last + j] = ship(column_sum(j), last + j, 8 * j)

    for place, j in enumerate(far):
        to_partner(j)
        if place:
            to_sides(far[place - 1])
    to_sides(0)
    for j in far:
        along(j)
    value = column_sum(0)
    for j in range(1, depth):
        value = arrived(value, last + j)
    body = value[0] / (total_members - 1.0)
    rim = value[1] / (total_members - 1.0)
    for t in range(lane_tiles):
        total_ref[t, 0:8, :] = rim[:, tile_cols(t)]
        total_ref[t, 8 : 8 + two, :] = body[:, tile_cols(t)]
        total_ref[t, 8 + two :, :] = rim[:, tile_cols(t)]
        stage_ref[0, t] = body[:, tile_cols(t)]
    wide = rows + 4
    for c in range(var_count):
        values = tile_rows(total_ref, pl.ds(4 + c, wide, stride=var_count))
        for b in range(3):
            moved = shifted(values, b)
            for t in range(lane_tiles):
                taps_ref[0, t, pl.ds(2 * b + c, wide, stride=8), :] = moved[:, tile_cols(t)]

    def tail_pair(p):
        for chunk in lane_chunks():
            lines = [(2 * p + line, t) for line, t in chunk]
            field = jnp.concatenate([tap_block(0, j, t) for j, t in lines], axis=1)
            tangent = jnp.dot(
                w_tail[...], field.astype(jnp.bfloat16), preferred_element_type=jnp.float32
            )
            slopes = jnp.concatenate([slopes_ref[j, :, tile_cols(t)] for j, t in lines], axis=1)
            back = (slopes * tangent).astype(jnp.bfloat16)
            for place, (j, t) in enumerate(lines):
                back_ref[j, :hidden, tile_cols(t)] = back[:, tile_cols(place)]

    in_groups(tail_pair, 0, pairs, TAIL_GROUP)
    in_groups(functools.partial(project_pair, v_tail[...]), 0, pairs, TAIL_GROUP)
    gather_pieces()
    for c in range(var_count):
        values = tile_rows(total_ref, pl.ds(8 + c, rows, stride=var_count)) + assembled(c)
        for t in range(lane_tiles):
            stage_ref[1, t, pl.ds(c, rows, stride=var_count), :] = values[:, tile_cols(t)]
    for copy in reduce_sends:
        copy.wait_send()


def emit_kernel(tiled_ref, incr_hbm, resp_hbm, out_sem):
    _, tiles, two, _ = tiled_ref.shape
    stores = []
    for index, target in enumerate((incr_hbm, resp_hbm)):
        for t in range(tiles):
            copy = pltpu.make_async_copy(
                tiled_ref.at[index, t],
                target.reshape(two, tiles * LANES).at[:, tile_cols(t)],
                out_sem.at[index, t],
            )
            copy.start()
            stores.append(copy)
    for copy in stores:
        copy.wait()


def whole_step(members, state, cotangent, conv_in, conv_out, bias):
    count = lax.axis_size("space")
    mine, lons, var_count, lats = members.shape
    rows = state.shape[0]
    hidden = bias.shape[0]
    two = rows * var_count
    tiles = lats // LANES
    depth = count // 8
    any_space = pl.BlockSpec(memory_space=pl.ANY)
    vmem = pltpu.VMEM
    dma = pltpu.SemaphoreType.DMA
    margin = HALF * var_count
    window = lats - LANES
    slots = 8 * depth
    tiled = pl.pallas_call(
        functools.partial(step_kernel, count, mine * count),
        out_shape=jax.ShapeDtypeStruct((2, tiles, two, LANES), jnp.float32),
        in_specs=[any_space] * 6,
        out_specs=pl.BlockSpec(memory_space=vmem),
        scratch_shapes=[
            vmem((mine, tiles, lons * var_count, LANES), jnp.bfloat16),
            vmem((2, tiles, two, LANES), jnp.float32),
            vmem((2, 2, tiles, 8, LANES), jnp.float32),
            vmem((2, tiles, (rows + 5) * 8, LANES), jnp.float32),
            vmem((2, 3, 3, var_count, hidden), jnp.float32),
            vmem((1, hidden), jnp.float32),
            vmem((4, 32, hidden), jnp.float32),
            vmem((hidden, 96), jnp.bfloat16),
            vmem((hidden, 96), jnp.bfloat16),
            vmem((64, 2 * hidden), jnp.bfloat16),
            vmem((hidden, 32), jnp.bfloat16),
            vmem((32, hidden), jnp.bfloat16),
            vmem((rows + 2, hidden, lats), jnp.float32),
            vmem((rows + 2, 2 * hidden, lats), jnp.bfloat16),
            vmem((rows + 2, 24, lats), jnp.float32),
            vmem((tiles, rows * 8, LANES), jnp.float32),
            vmem((tiles, two, LANES), jnp.float32),
            vmem((count, two, lats), jnp.bfloat16),
            vmem((2, window, window), jnp.bfloat16),
            vmem((4 * two, 4 * two + 2 * margin), jnp.bfloat16),
            vmem((16, 2 * (margin + 16)), jnp.bfloat16),
            vmem((lons * var_count + 2 * (margin + 16), mine * lats), jnp.bfloat16),
            vmem((lons * var_count + 16, lats), jnp.float32),
            vmem((slots, two + 8, lats), jnp.bfloat16),
            vmem((slots, two + 8, lats), jnp.bfloat16),
            vmem((tiles, two + 16, LANES), jnp.float32),
            dma((mine, tiles)),
            dma((2, tiles)),
            dma((3,)),
            dma((2,)),
            dma((2,)),
            dma((count,)),
            dma((count,)),
            dma((slots,)),
            dma((slots,)),
        ],
        compiler_params=pltpu.CompilerParams(collective_id=2, has_side_effects=True),
        name="whole_step",
    )(
        members,
        state,
        cotangent,
        jnp.transpose(conv_in, (0, 1, 3, 2)),
        conv_out,
        bias.reshape(1, hidden),
    )
    return pl.pallas_call(
        emit_kernel,
        out_shape=(jax.ShapeDtypeStruct(state.shape, jnp.float32),) * 2,
        in_specs=[pl.BlockSpec(memory_space=vmem)],
        out_specs=(any_space,) * 2,
        scratch_shapes=[dma((2, tiles))],
        name="emit",
    )(tiled)


def fits(members, state, bias):
    count = lax.axis_size("space")
    mine, lons, var_count, lats = members.shape
    rows = state.shape[0]
    return (
        lax.axis_size("mem") == 1
        and count >= 8
        and count & (count - 1) == 0
        and var_count == 2
        and lats == 3 * LANES
        and rows % 8 == 0
        and rows >= 2 * 8
        and mine % 2 == 0
        and lons == count * rows
        and bias.shape[0] == LANES
    )


def per_device(members, state, cotangent, conv_in, conv_out, bias):
    row_count, var_count, lat_count = state.shape
    if fits(members, state, bias):
        return whole_step(members, state, cotangent, conv_in, conv_out, bias)
    count = lax.axis_size("space")
    direct = count >= 8 and count & (count - 1) == 0
    rim_width = 2
    joined = jnp.concatenate([state, cotangent], axis=1)
    padded = padded_2(joined, "space", rim_width)
    state_pad = padded[:, :var_count]
    cot_pad = padded[:, var_count:]
    activity = jnp.tanh(convolve_fine(state_pad, conv_in) + bias[None, :, None])
    slopes = 1.0 - activity * activity
    backward = slopes * convolve_fine(cot_pad, flipped(conv_out))
    gradient = cotangent + convolve_fine(backward, flipped(conv_in))
    gradient = gradient.astype(jnp.bfloat16)
    width = var_count * lat_count
    gradient = gradient.reshape(row_count, width)
    if direct:
        whole = gather(gradient).reshape(count * row_count, width)
    else:
        whole = lax.all_gather(gradient, "space", axis=0, tiled=True)
    merged = members.reshape(members.shape[0], members.shape[1], width)
    lat_loc = band_matrix(lat_count, False)
    lon_loc = band_matrix(merged.shape[1], True)
    contrib = covariance(merged, whole, lat_loc, lon_loc)
    member_count = members.shape[0] * lax.axis_size("space") * lax.axis_size("mem")
    if direct:
        own, left, right = scatter(
            contrib.reshape(count, row_count, width), rim_width
        )
        total = jnp.concatenate([left, own, right], axis=0)
        total = total.reshape(row_count + 2 * rim_width, var_count, lat_count)
        if lax.axis_size("mem") > 1:
            total = lax.psum(total, "mem")
        incr_pad = total / (member_count - 1.0)
        increment = incr_pad[rim_width : rim_width + row_count]
    else:
        member_sum = lax.psum(contrib, "mem")
        block_sum = lax.psum_scatter(member_sum, "space", scatter_dimension=0, tiled=True)
        increment = block_sum.reshape(state.shape) / (member_count - 1.0)
        incr_pad = padded_2(increment, "space", rim_width)
    tangent_hidden = slopes * convolve(incr_pad, conv_in)
    response = increment + convolve(tangent_hidden, conv_out)
    return (increment, response)


def solution(mesh):
    in_specs = (
        P(("space", "mem"), None, None, None),
        P("space", None, None),
        P("space", None, None),
        P(),
        P(),
        P(),
    )
    out_specs = (P("space", None, None), P("space", None, None))
    return jax.shard_map(
        per_device, mesh=mesh, in_specs=in_specs, out_specs=out_specs, check_vma=False
    )
```
